32 devices in a mesh: batch: 4 (over x, core), seq: 2 (over y), heads: 4 (over z).
Axes of the slice: x: 2, y: 2, z: 4, core: 2. Of those that a mesh axis runs over, the one named last changes fastest.
Arguments:
- hidden_in: bfloat16 [48, 5120], P('batch', 'seq'), may hold values from -7 to 7
- lengths: int32 [48], P('batch'), may hold values from 1 to 512
- draft_ids: int32 [48], P('batch'), may hold values from 0 to 31999
- input_gain: float32 [5120], P('seq'), may hold values from 0.5 to 1.5
- w_query: bfloat16 [5120, 5120], P('seq', 'heads'), may hold values from -0.078125 to 0.078125
- w_latent: bfloat16 [5120, 4, 640], P('seq', 'heads'), may hold values from -0.078125 to 0.078125
- latent_cache: bfloat16 [48, 4, 512, 640], P('batch', 'heads', 'seq'), may hold values from -1200 to 1200
- key_up: bfloat16 [4, 320, 1280], P('heads'), may hold values from -0.3125 to 0.3125
- value_up: bfloat16 [4, 320, 1280], P('heads'), may hold values from -0.3125 to 0.3125
- w_out: bfloat16 [5120, 5120], P('heads', 'seq'), may hold values from -0.078125 to 0.078125
- final_gain: float32 [5120], P('seq'), may hold values from 0.1 to 1.9
- w_vocab: bfloat16 [5120, 32000], P('seq', 'heads'), may hold values from -0.26 to 0.26
Outputs:
- new_hidden: bfloat16 [48, 5120], P('batch', 'seq')
- log_probs: float32 [48, 32000], P('batch', 'heads')
- draft_logprob: float32 [48], P('batch')
The draws below stay inside these ranges and needn't reach their ends.
Inputs may be any that keep to these rules, and one draw needn't show every extreme that they name: `lengths`: cache positions below a request's length are its live context.
All inputs are finite; a program needn't handle non-finite values.
Results may differ from the reference program's by a relative error of at most 0.012.
The reference program's roundings to bfloat16 on the way count: a program that leaves them out, or rounds other values in their place, can miss the bound.
Values sent between devices are 32-bit elements; how exact they have to be, the bound alone decides.
No kernel may reach another device: no remote copies, remote signals or barrier semaphores. Data moves between devices by JAX's collectives and lax.ppermute only.
A program may use at most 128 MiB of HBM per device.

```python
import math
import jax
import jax.numpy as jnp
from jax import lax

D = 5120
HEADS = 40
HEAD_DIM = 128
VOCAB = 32000
GROUP_HEADS = 10
GROUP_RANK = 320
BATCH = 48
CONTEXT = 512
GROUPS = 4


planted_pairs = 4


def hidden_rows(key):
    value_key = jax.random.fold_in(jax.random.fold_in(key, 11), 0)
    return jnp.clip(jax.random.normal(value_key, (BATCH, D), jnp.float32), -6.0, 6.0)


def draw_hidden_in(key, part):
    return hidden_rows(key).astype(jnp.bfloat16)


def draw_w_vocab(key, part):
    subkeys = jax.random.split(jax.random.fold_in(key, 23), 1)
    base = jnp.clip(jax.random.normal(subkeys[0], (D, VOCAB), jnp.float32), -6.0, 6.0)
    rising = jnp.exp(jnp.linspace(0.0, math.log(2.5), VOCAB, dtype=jnp.float32))
    table = base * float(D) ** (-0.5) * rising[None, :]
    return table.astype(jnp.bfloat16)


def drawn_spots(subkey):
    return jax.random.permutation(subkey, CONTEXT)[:2 * planted_pairs]


def planted_table(key):
    subkeys = jax.random.split(key, 6)
    shape = (BATCH, CONTEXT, 2 * GROUP_RANK)
    table = jnp.clip(jax.random.normal(subkeys[0], shape, jnp.float32), -6.0, 6.0)
    chosen = jax.random.bernoulli(subkeys[1], 0.4, (BATCH,))
    spots = jax.vmap(drawn_spots)(jax.random.split(subkeys[2], BATCH))
    strength = jnp.exp(jax.random.uniform(subkeys[3], (BATCH, planted_pairs, 1), jnp.float32, math.log(120.0), math.log(300.0)))
    direction = jnp.clip(jax.random.normal(subkeys[4], (BATCH, planted_pairs, GROUP_RANK), jnp.float32), -4.0, 4.0)
    shrink = jax.random.uniform(subkeys[5], (BATCH, planted_pairs, 1), jnp.float32, 0.005, 0.01)
    first_keys = strength * direction
    second_keys = first_keys * (1.0 - shrink)
    planted = jnp.concatenate([first_keys, second_keys], axis=1)
    request_index = jnp.arange(BATCH, dtype=jnp.int32)[:, None]
    current = table[request_index, spots, :GROUP_RANK]
    table = table.at[request_index, spots, :GROUP_RANK].set(jnp.where(chosen[:, None, None], planted, current))
    return table


def draw_latent_cache(key, part):
    groups_list = [planted_table(jax.random.fold_in(key, 101 + index)).astype(jnp.bfloat16) for index in range(GROUPS)]
    return jnp.stack(groups_list, axis=1)


def place_ends(values, rng, smallest, high):
    spot = [jax.random.randint(jax.random.fold_in(rng, axis), (), 0, length) for axis, length in enumerate(values.shape)]
    widest = values.shape.index(max(values.shape))
    beside = spot[:widest] + [(spot[widest] + 1) % values.shape[widest]] + spot[widest + 1:]
    return values.at[tuple(spot)].set(smallest).at[tuple(beside)].set(high)


def shard_levels(stream_key, dims, cuts, least, largest):
    loudness, own = 1.0, jax.random.fold_in(stream_key, 6)
    for axis_at, shards_of in cuts:
        heights = jnp.exp(jax.random.uniform(jax.random.fold_in(own, axis_at), (shards_of,), jnp.float32, least / len(cuts), largest / len(cuts)))
        loudness = loudness * jnp.repeat(heights, dims[axis_at] // shards_of).reshape([-1 if axis == axis_at else 1 for axis in range(len(dims))])
    return loudness


def bell_draw(key, extent, deviation, limit, cuts=(), held_as=jnp.bfloat16):
    result = jax.random.normal(key, extent, jnp.float32) * deviation
    if len(cuts) > 0:
        result = shard_levels(key, extent, cuts, -0.22, 0.18) * result
    return jnp.clip(result, min=-limit, max=limit).astype(held_as)


def setup_inputs(seed: int = 0) -> dict:
    streams_of = jax.random.split(jax.random.key(seed), 13)
    hidden_in = draw_hidden_in(jax.random.fold_in(streams_of[12], 71), 0)
    lengths = place_ends(jax.random.randint(streams_of[1], (BATCH,), 1, CONTEXT + 1), jax.random.fold_in(streams_of[1], 1), 1, CONTEXT).astype(jnp.int32)
    draft_ids = place_ends(jax.random.randint(streams_of[2], (BATCH,), 0, VOCAB), jax.random.fold_in(streams_of[2], 1), 0, VOCAB - 1).astype(jnp.int32)
    input_gain = jnp.clip(1.0 + 0.1 * jax.random.normal(streams_of[3], (D,), jnp.float32), 0.5, 1.5)
    w_query = bell_draw(streams_of[4], (D, HEADS * HEAD_DIM), D ** -0.5, 0.078125, ((0, 2), (1, 4)))
    w_latent = bell_draw(streams_of[5], (D, GROUPS, 2 * GROUP_RANK), D ** -0.5, 0.078125, ((0, 2), (1, 4)))
    latent_cache = draw_latent_cache(jax.random.fold_in(streams_of[12], 71), 0)
    key_up = bell_draw(streams_of[7], (GROUPS, GROUP_RANK, GROUP_HEADS * HEAD_DIM), GROUP_RANK ** -0.5, 0.3125, ((0, 4),))
    value_up = bell_draw(streams_of[8], (GROUPS, GROUP_RANK, GROUP_HEADS * HEAD_DIM), GROUP_RANK ** -0.5, 0.3125, ((0, 4),))
    w_out = bell_draw(streams_of[9], (HEADS * HEAD_DIM, D), (HEADS * HEAD_DIM) ** -0.5, 0.078125, ((0, 4), (1, 2)))
    final_gain = jnp.clip(1.0 + 0.18 * jax.random.normal(streams_of[10], (D,), jnp.float32), 0.1, 1.9)
    w_vocab = draw_w_vocab(jax.random.fold_in(streams_of[12], 71), 0)
    return {"hidden_in": hidden_in, "lengths": lengths, "draft_ids": draft_ids, "input_gain": input_gain, "w_query": w_query, "w_latent": w_latent, "latent_cache": latent_cache, "key_up": key_up, "value_up": value_up, "w_out": w_out, "final_gain": final_gain, "w_vocab": w_vocab}


epsilon = 1e-05
negative_fill = -1e+30

def attend_group(query_group, latent_group, cache_slab, key_map, value_map, lengths):
    batch_rows = query_group.shape[0]
    scaling = 1.0 / math.sqrt(HEAD_DIM)
    highest_prec = lax.Precision.HIGHEST
    heads_query = query_group.reshape(batch_rows, GROUP_HEADS, HEAD_DIM).astype(jnp.float32)
    key_table = key_map.astype(jnp.float32).reshape(GROUP_RANK, GROUP_HEADS, HEAD_DIM)
    absorbed_low = jnp.einsum('bhd,rhd->bhr', heads_query, key_table, precision=highest_prec).astype(jnp.bfloat16)
    absorbed = lax.optimization_barrier(absorbed_low).astype(jnp.float32)
    key_rows = cache_slab[:, :, :GROUP_RANK].astype(jnp.float32)
    value_rows = cache_slab[:, :, GROUP_RANK:].astype(jnp.float32)
    scores = jnp.einsum('bhr,btr->bht', absorbed, key_rows, precision=highest_prec) * scaling
    positions = jnp.arange(CONTEXT, dtype=jnp.int32)
    live_mask = positions[None, None, :] < lengths[:, None, None]
    scores = jnp.where(live_mask, scores, negative_fill)
    own_key = latent_group[:, :GROUP_RANK].astype(jnp.float32)
    own_value = latent_group[:, GROUP_RANK:].astype(jnp.float32)
    own_score = jnp.einsum('bhr,br->bh', absorbed, own_key, precision=highest_prec) * scaling
    highest = jnp.maximum(lax.optimization_barrier(jnp.max(scores, axis=2)), own_score)
    weights = jnp.where(live_mask, jnp.exp(scores - highest[..., None]), 0.0)
    own_weight = jnp.exp(own_score - highest)
    denominator = lax.optimization_barrier(jnp.sum(weights, axis=2)) + own_weight
    rounded = lax.optimization_barrier(weights.astype(jnp.bfloat16)).astype(jnp.float32)
    mixed_sum = jnp.einsum('bht,btr->bhr', rounded, value_rows, precision=highest_prec)
    mixed_sum = mixed_sum + own_weight[..., None] * own_value[:, None, :]
    latent_out = mixed_sum / denominator[..., None]
    value_table = value_map.astype(jnp.float32).reshape(GROUP_RANK, GROUP_HEADS, HEAD_DIM)
    head_out = jnp.einsum('bhr,rhd->bhd', latent_out, value_table, precision=highest_prec).astype(jnp.bfloat16)
    return head_out.reshape(batch_rows, GROUP_HEADS * HEAD_DIM)

def reference(hidden_in, lengths, draft_ids, input_gain, w_query, w_latent, latent_cache, key_up, value_up, w_out, final_gain, w_vocab):
    states = hidden_in.astype(jnp.float32)
    inv_rms = lax.rsqrt(lax.optimization_barrier(jnp.mean(states * states, axis=1, keepdims=True)) + epsilon)
    gained = (states * input_gain).astype(jnp.bfloat16)
    query_rows = (inv_rms * jnp.dot(gained, w_query, preferred_element_type=jnp.float32)).astype(jnp.bfloat16)
    latent_matrix = w_latent.reshape(D, GROUPS * 2 * GROUP_RANK)
    latent = (inv_rms * jnp.dot(gained, latent_matrix, preferred_element_type=jnp.float32)).astype(jnp.bfloat16)
    head_width = GROUP_HEADS * HEAD_DIM
    latent_width = 2 * GROUP_RANK
    pieces = []
    for group_idx in range(GROUPS):
        pieces.append(attend_group(query_rows[:, group_idx * head_width:(group_idx + 1) * head_width], latent[:, group_idx * latent_width:(group_idx + 1) * latent_width], latent_cache[:, group_idx], key_up[group_idx], value_up[group_idx], lengths))
    heads_out = jnp.concatenate(pieces, axis=1)
    updated = states + jnp.dot(heads_out, w_out, preferred_element_type=jnp.float32)
    new_hidden = updated.astype(jnp.bfloat16)
    inv_final = lax.rsqrt(lax.optimization_barrier(jnp.mean(updated * updated, axis=1, keepdims=True)) + epsilon)
    final_scaled = (updated * final_gain).astype(jnp.bfloat16)
    logits = inv_final * jnp.dot(final_scaled, w_vocab, preferred_element_type=jnp.float32)
    highest = lax.optimization_barrier(jnp.max(logits, axis=1, keepdims=True))
    log_total = highest + jnp.log(lax.optimization_barrier(jnp.sum(jnp.exp(logits - highest), axis=1, keepdims=True)))
    log_probs = logits - log_total
    picked = jnp.take_along_axis(logits, draft_ids[:, None].astype(jnp.int32), axis=1)[:, 0]
    draft_logprob = picked - log_total[:, 0]
    return (new_hidden, log_probs, draft_logprob)
```

```python
import math

import jax
import jax.numpy as jnp
from jax import lax
from jax.experimental import pallas as pl
from jax.experimental.pallas import tpu as pltpu
from jax.sharding import PartitionSpec as P

HEAD_DIM = 128
LANES = 128
ROW_TILE = 16
EPSILON = 1e-05
NEGATIVE = -1e30
MIB = 1 << 20
ANY = pl.BlockSpec(memory_space=pl.ANY)
VMEM = pl.BlockSpec(memory_space=pltpu.VMEM)
SMEM = pl.BlockSpec(memory_space=pltpu.SMEM)
NT = (((1,), (1,)), ((), ()))


def resident(array):
    return pltpu.with_memory_space_constraint(array, pltpu.VMEM)


def stored(array):
    return pltpu.with_memory_space_constraint(array, pltpu.HBM)


def cost(micros):
    return pl.CostEstimate(flops=int(micros * 5e6), bytes_accessed=0, transcendentals=0)


def params(mib):
    return pltpu.CompilerParams(vmem_limit_bytes=int(mib * MIB))


def round_up(value, step):
    return -(-value // step) * step


def fold_of(rows, width):
    fold = 8 // math.gcd(rows, 8)
    return fold if width % (fold * LANES) == 0 else 1


def put_folded(ref, rows, fold, start, value):
    width = ref.shape[1]
    done = 0
    while done < value.shape[1]:
        piece, at = divmod(start + done, width)
        size = min(value.shape[1] - done, width - at)
        ref[piece * rows : (piece + 1) * rows, at : at + size] = value[:, done : done + size]
        done += size


def get_folded(refs, rows, start, size):
    width = refs[0].shape[1]
    pieces = []
    done = 0
    while done < size:
        piece, at = divmod(start + done, width)
        span = min(size - done, width - at)
        block = None
        for ref in refs:
            term = ref[piece * rows : (piece + 1) * rows, at : at + span]
            block = term if block is None else block + term
        pieces.append(block)
        done += span
    return pieces[0] if len(pieces) == 1 else jnp.concatenate(pieces, axis=1)


def swap(array, axis, mask):
    size = lax.axis_size(axis)
    return lax.ppermute(array, axis, [(i, i ^ mask) for i in range(size)])


def is_power(size):
    return size & (size - 1) == 0


def project(hidden, gain, w_query, w_latent):
    rows, depth = hidden.shape
    q_width, l_width = w_query.shape[1], w_latent.shape[1]
    width = q_width + l_width + LANES
    fold = fold_of(rows, width)
    chunks = 5 if depth % (5 * LANES) == 0 else 1
    step = depth // chunks

    def kernel(x_ref, gain_ref, wq_ref, wl_ref, out_ref, q_buf, l_buf, sems):
        copies = []
        for c in range(chunks):
            at = pl.ds(c * step, step)
            copies.append(
                (
                    pltpu.make_async_copy(wq_ref.at[at], q_buf.at[at], sems.at[0, c]),
                    pltpu.make_async_copy(wl_ref.at[at], l_buf.at[at], sems.at[1, c]),
                )
            )
        for pair in copies:
            for copy in pair:
                copy.start()
        states = x_ref[...].astype(jnp.float32)
        gained = (states * gain_ref[...]).astype(jnp.bfloat16)
        square = jnp.sum(states * states, axis=1, keepdims=True)
        acc_q = acc_l = None
        for c in range(chunks):
            for copy in copies[c]:
                copy.wait()
            x = gained[:, c * step : (c + 1) * step]
            part_q = jnp.dot(
                x, q_buf[c * step : (c + 1) * step, :], preferred_element_type=jnp.float32
            )
            part_l = jnp.dot(
                x, l_buf[c * step : (c + 1) * step, :], preferred_element_type=jnp.float32
            )
            acc_q = part_q if c == 0 else acc_q + part_q
            acc_l = part_l if c == 0 else acc_l + part_l
        put_folded(out_ref, rows, fold, 0, acc_q)
        put_folded(out_ref, rows, fold, q_width, acc_l)
        put_folded(
            out_ref, rows, fold, q_width + l_width, jnp.broadcast_to(square, (rows, LANES))
        )

    return pl.pallas_call(
        kernel,
        out_shape=jax.ShapeDtypeStruct((rows * fold, width // fold), jnp.float32),
        in_specs=[VMEM, VMEM, ANY, ANY],
        out_specs=VMEM,
        scratch_shapes=[
            pltpu.VMEM(w_query.shape, w_query.dtype),
            pltpu.VMEM(w_latent.shape, w_latent.dtype),
            pltpu.SemaphoreType.DMA((2, chunks)),
        ],
        compiler_params=params(14),
        cost_estimate=cost(5),
        name="project",
    )(hidden, gain, stored(w_query), stored(w_latent))


def fetch_rows(table, after, low, high, micros, pieces=4):
    step = round_up(-(-(high - low) // pieces), 16)
    bounds = [(at, min(at + step, high)) for at in range(low, high, step)]

    def kernel(table_ref, after_ref, out_ref, sems):
        copies = [
            pltpu.make_async_copy(
                table_ref.at[pl.ds(a, b - a)], out_ref.at[pl.ds(a - low, b - a)], sems.at[i]
            )
            for i, (a, b) in enumerate(bounds)
        ]
        for copy in copies:
            copy.start()
        for copy in copies:
            copy.wait()

    return pl.pallas_call(
        kernel,
        out_shape=pltpu.VMEM((high - low,) + table.shape[1:], table.dtype),
        in_specs=[ANY, ANY],
        out_specs=VMEM,
        scratch_shapes=[pltpu.SemaphoreType.DMA((len(bounds),))],
        compiler_params=params(1),
        cost_estimate=cost(micros),
        name="fetch_rows",
    )(stored(table), after)


def fetch_attention(cache, key_up, value_up, after, micros):
    rank, width = value_up.shape
    full = round_up(rank, LANES)

    def kernel(cache_ref, key_ref, value_ref, after_ref, cache_out, key_out, value_out, sems):
        requests = cache.shape[0]
        copies = [
            pltpu.make_async_copy(key_ref, key_out, sems.at[0]),
            pltpu.make_async_copy(value_ref, value_out.at[pl.ds(full - rank, rank)], sems.at[1]),
            pltpu.make_async_copy(cache_ref, cache_out, sems.at[2]),
        ]
        for copy in copies:
            copy.start()
        value_out[0 : full - rank, :] = jnp.zeros((full - rank, width), value_up.dtype)
        for copy in copies:
            copy.wait()

    return pl.pallas_call(
        kernel,
        out_shape=(
            pltpu.VMEM(cache.shape, cache.dtype),
            pltpu.VMEM(key_up.shape, key_up.dtype),
            pltpu.VMEM((full, width), value_up.dtype),
        ),
        in_specs=[ANY] * 4,
        out_specs=(VMEM,) * 3,
        scratch_shapes=[pltpu.SemaphoreType.DMA((3,))],
        compiler_params=params(1),
        cost_estimate=cost(micros),
        name="fetch_attention",
    )(stored(cache), stored(key_up), stored(value_up), after)


def attend(own, other, lengths, cache, key_up, value_pad, features):
    requests, span, width = cache.shape
    rank = width // 2
    full = value_pad.shape[0]
    low = width - full
    heads = key_up.shape[1] // HEAD_DIM
    slot = round_up(heads, 8)
    scaling = 1.0 / math.sqrt(HEAD_DIM)
    q_width = heads * HEAD_DIM
    send_width = q_width + 2 * LANES
    fold = fold_of(requests, send_width)

    def kernel(
        own_ref, other_ref, length_ref, cache_ref, key_ref, value_ref,
        send_ref, local_ref, score_own, top_buf, total_buf, latent_buf, stack, *tiles,
    ):
        absorbed, mixed = tiles[: full // LANES], tiles[full // LANES :]
        refs = (own_ref, other_ref)
        square = get_folded(refs, requests, q_width + width, LANES)
        inv = lax.rsqrt(square[:, 0:1] / features + EPSILON)
        query = (inv * get_folded(refs, requests, 0, q_width)).astype(jnp.bfloat16)
        latent = (inv * get_folded(refs, requests, q_width, width)).astype(jnp.bfloat16)
        latent_buf[...] = latent.astype(jnp.float32)
        for tile in absorbed:
            tile[...] = jnp.zeros(tile.shape, jnp.float32)
        for j in range(heads):
            at = slice(j * HEAD_DIM, (j + 1) * HEAD_DIM)
            row = lax.dot_general(
                query[:, at], key_ref[:, at], NT, preferred_element_type=jnp.float32
            )
            row = row.astype(jnp.bfloat16).astype(jnp.float32)
            for i, tile in enumerate(absorbed):
                piece = row[:, i * LANES : min((i + 1) * LANES, rank)]
                if piece.shape[1] < LANES:
                    edge = jnp.zeros((requests, LANES - piece.shape[1]), jnp.float32)
                    piece = jnp.concatenate([piece, edge], axis=1)
                tile[pl.ds(j, requests, stride=slot), :] = piece
        first = lax.axis_index("seq") * span
        positions = first + lax.broadcasted_iota(jnp.int32, (slot, span), 1)
        for b in range(requests):
            at = slice(b * slot, (b + 1) * slot)
            rows = jnp.concatenate([tile[at, :] for tile in absorbed], axis=1)
            score_own[at, :] = jnp.broadcast_to(
                jnp.sum(rows * latent_buf[b : b + 1, 0:full], axis=1, keepdims=True) * scaling,
                (slot, LANES),
            )
            scores = (
                lax.dot_general(
                    rows.astype(jnp.bfloat16),
                    cache_ref[b, :, 0:full],
                    NT,
                    preferred_element_type=jnp.float32,
                )
                * scaling
            )
            live = positions < length_ref[b]
            scores = jnp.where(live, scores, NEGATIVE)
            top = jnp.max(scores, axis=1, keepdims=True)
            weights = jnp.where(live, jnp.exp(scores - top), 0.0)
            top_buf[at, :] = jnp.broadcast_to(top, (slot, LANES))
            total_buf[at, :] = jnp.broadcast_to(
                jnp.sum(weights, axis=1, keepdims=True), (slot, LANES)
            )
            value = jnp.dot(
                weights.astype(jnp.bfloat16),
                cache_ref[b, :, low:width],
                preferred_element_type=jnp.float32,
            )
            for i, tile in enumerate(mixed):
                tile[at, :] = value[:, i * LANES : (i + 1) * LANES]
        lane = lax.broadcasted_iota(jnp.int32, (requests, LANES), 1)
        tops = jnp.full((requests, LANES), NEGATIVE, jnp.float32)
        owns = jnp.full((requests, LANES), NEGATIVE, jnp.float32)
        totals = jnp.zeros((requests, LANES), jnp.float32)
        second = ROW_TILE * -(-requests // ROW_TILE)
        stack[2 * second : 2 * second + requests, :] = latent[:, low:width]
        for j in range(heads):
            pick = pl.ds(j, requests, stride=slot)
            tops = jnp.where(lane == j, top_buf[pick, :], tops)
            totals = jnp.where(lane == j, total_buf[pick, :], totals)
            owns = jnp.where(lane == j, score_own[pick, :], owns)
            value = jnp.concatenate([tile[pick, :] for tile in mixed], axis=1)
            high = value.astype(jnp.bfloat16)
            stack[0:requests, :] = high
            stack[second : second + requests, :] = (value - high.astype(jnp.float32)).astype(
                jnp.bfloat16
            )
            at = slice(j * HEAD_DIM, (j + 1) * HEAD_DIM)
            lifted = jnp.dot(stack[...], value_ref[:, at], preferred_element_type=jnp.float32)
            put_folded(
                send_ref, requests, fold, j * HEAD_DIM,
                lifted[0:requests] + lifted[second : second + requests],
            )
            local_ref[:, at] = lifted[2 * second : 2 * second + requests]
        put_folded(send_ref, requests, fold, q_width, tops)
        put_folded(send_ref, requests, fold, q_width + LANES, totals)
        local_ref[:, q_width : q_width + LANES] = owns

    tall = requests * slot
    return pl.pallas_call(
        kernel,
        out_shape=(
            jax.ShapeDtypeStruct((requests * fold, send_width // fold), jnp.float32),
            jax.ShapeDtypeStruct((requests, q_width + LANES), jnp.float32),
        ),
        in_specs=[VMEM, VMEM, SMEM, VMEM, VMEM, VMEM],
        out_specs=(VMEM, VMEM),
        scratch_shapes=[
            pltpu.VMEM((tall, LANES), jnp.float32),
            pltpu.VMEM((tall, LANES), jnp.float32),
            pltpu.VMEM((tall, LANES), jnp.float32),
            pltpu.VMEM((requests, width), jnp.float32),
            pltpu.VMEM((3 * round_up(requests, ROW_TILE), full), jnp.bfloat16),
        ]
        + [pltpu.VMEM((tall, LANES), jnp.float32)] * (2 * full // LANES),
        compiler_params=params(5),
        cost_estimate=cost(5),
        name="attend",
    )(own, other, lengths, resident(cache), resident(key_up), resident(value_pad))


def merge_out(own, other, local, w_out, requests):
    q_width = local.shape[1] - LANES
    heads = q_width // HEAD_DIM
    width = w_out.shape[1]
    fold = fold_of(requests, width)
    step = 512 if width % 512 == 0 else width

    def kernel(own_ref, other_ref, local_ref, w_ref, out_ref, head_buf):
        top_a = get_folded((own_ref,), requests, q_width, LANES)
        top_b = get_folded((other_ref,), requests, q_width, LANES)
        total_a = get_folded((own_ref,), requests, q_width + LANES, LANES)
        total_b = get_folded((other_ref,), requests, q_width + LANES, LANES)
        own_score = local_ref[:, q_width : q_width + LANES]
        highest = jnp.maximum(jnp.maximum(top_a, top_b), own_score)
        scale_a = jnp.exp(top_a - highest)
        scale_b = jnp.exp(top_b - highest)
        own_weight = jnp.exp(own_score - highest)
        below = total_a * scale_a + total_b * scale_b + own_weight
        scale_a = scale_a / below
        scale_b = scale_b / below
        own_weight = own_weight / below
        for j in range(heads):
            at = slice(j * HEAD_DIM, (j + 1) * HEAD_DIM)
            value = (
                get_folded((own_ref,), requests, j * HEAD_DIM, HEAD_DIM) * scale_a[:, j : j + 1]
                + get_folded((other_ref,), requests, j * HEAD_DIM, HEAD_DIM)
                * scale_b[:, j : j + 1]
                + local_ref[:, at] * own_weight[:, j : j + 1]
            )
            head_buf[:, at] = value.astype(jnp.bfloat16)
        head_out = head_buf[...]
        for at in range(0, width, step):
            put_folded(
                out_ref, requests, fold, at,
                jnp.dot(head_out, w_ref[:, at : at + step], preferred_element_type=jnp.float32),
            )

    return pl.pallas_call(
        kernel,
        out_shape=jax.ShapeDtypeStruct((requests * fold, width // fold), jnp.float32),
        in_specs=[VMEM] * 4,
        out_specs=VMEM,
        scratch_shapes=[pltpu.VMEM((requests, q_width), jnp.bfloat16)],
        compiler_params=params(3),
        cost_estimate=cost(2),
        name="merge_out",
    )(own, other, local, resident(w_out))


def finish_states(own, other, hidden, gain):
    rows, width = hidden.shape

    def kernel(own_ref, other_ref, x_ref, gain_ref, new_ref, scaled_ref, square_ref):
        states = x_ref[...].astype(jnp.float32)
        updated = states + get_folded((own_ref, other_ref), rows, 0, width)
        new_ref[...] = updated.astype(jnp.bfloat16)
        scaled_ref[...] = (updated * gain_ref[...]).astype(jnp.bfloat16)
        square_ref[...] = jnp.broadcast_to(
            jnp.sum(updated * updated, axis=1, keepdims=True), (rows, LANES)
        )

    return pl.pallas_call(
        kernel,
        out_shape=(
            jax.ShapeDtypeStruct((rows, width), jnp.bfloat16),
            jax.ShapeDtypeStruct((rows, width), jnp.bfloat16),
            jax.ShapeDtypeStruct((rows, LANES), jnp.float32),
        ),
        in_specs=[VMEM] * 4,
        out_specs=(VMEM,) * 3,
        compiler_params=params(2),
        cost_estimate=cost(1),
        name="finish_states",
    )(own, other, hidden, gain)


def vocab_part(scaled, square, tables, first, last, width):
    rows = scaled.shape[0]
    fold = fold_of(rows, width)
    step = 512

    def kernel(x_ref, square_ref, *refs):
        tables_in, out_ref = refs[:-1], refs[-1]
        x = x_ref[...]
        base = 0
        for table in tables_in:
            low, high = max(first, base), min(last, base + table.shape[0])
            for at in range(low, high, step):
                end = min(at + step, high)
                put_folded(
                    out_ref, rows, fold, at - first,
                    lax.dot_general(
                        x, table[at - base : end - base, :], NT,
                        preferred_element_type=jnp.float32,
                    ),
                )
            base += table.shape[0]
        if last - first < width:
            put_folded(
                out_ref, rows, fold, last - first,
                jnp.broadcast_to(square_ref[:, 0:1], (rows, width - (last - first))),
            )

    return pl.pallas_call(
        kernel,
        out_shape=jax.ShapeDtypeStruct((rows * fold, width // fold), jnp.float32),
        in_specs=[VMEM] * (2 + len(tables)),
        out_specs=VMEM,
        compiler_params=params(3),
        cost_estimate=cost(6),
        name="vocab_part",
    )(scaled, square, *[resident(table) for table in tables])


def vocab_logits(parts, draft_ids, bounds, rows, features):
    columns = bounds[-1][1]
    count = len(bounds)
    flat = [array for pair in parts for array in pair]

    def kernel(id_ref, *refs):
        pairs = [refs[2 * i : 2 * i + 2] for i in range(count)]
        logit_ref, stat_ref = refs[2 * count :]
        full = pairs[-1][0].shape[0] * pairs[-1][0].shape[1] // rows
        square = get_folded(pairs[-1], rows, full - LANES, LANES)
        inv = lax.rsqrt(square[:, 0:1] / features + EPSILON)
        row = lax.broadcasted_iota(jnp.int32, (rows, 1), 0)
        wanted = jnp.zeros((rows, 1), jnp.int32)
        for r in range(rows):
            wanted = jnp.where(row == r, id_ref[r], wanted)
        wanted = wanted - lax.axis_index("heads") * columns
        top = jnp.full((rows, 1), NEGATIVE, jnp.float32)
        picked = jnp.zeros((rows, 1), jnp.float32)
        for pair, (first, last) in zip(pairs, bounds):
            logits = get_folded(pair, rows, 0, last - first) * inv
            logit_ref[:, first:last] = logits
            top = jnp.maximum(top, jnp.max(logits, axis=1, keepdims=True))
            column = first + lax.broadcasted_iota(jnp.int32, logits.shape, 1)
            picked = picked + jnp.sum(
                jnp.where(column == wanted, logits, 0.0), axis=1, keepdims=True
            )
        total = jnp.zeros((rows, 1), jnp.float32)
        for first, last in bounds:
            total = total + jnp.sum(
                jnp.exp(logit_ref[:, first:last] - top), axis=1, keepdims=True
            )
        lane = lax.broadcasted_iota(jnp.int32, (rows, LANES), 1)
        stat_ref[...] = jnp.where(
            lane == 0, top, jnp.where(lane == 1, total, jnp.where(lane == 2, picked, 0.0))
        )

    return pl.pallas_call(
        kernel,
        out_shape=(
            pltpu.VMEM((rows, columns), jnp.float32),
            jax.ShapeDtypeStruct((rows, LANES), jnp.float32),
        ),
        in_specs=[SMEM] + [VMEM] * len(flat),
        out_specs=(VMEM, VMEM),
        compiler_params=params(4),
        cost_estimate=cost(2),
        name="vocab_logits",
    )(draft_ids, *flat)


def vocab_finish(logits, stats):
    rows, columns = logits.shape
    count = len(stats)

    def kernel(logit_ref, *refs):
        stat_refs, out_ref, draft_ref = refs[:count], refs[count], refs[count + 1]
        state = [(ref[:, 0:1], ref[:, 1:2], ref[:, 2:3]) for ref in stat_refs]
        while len(state) > 1:
            joined = []
            for (top_a, sum_a, pick_a), (top_b, sum_b, pick_b) in zip(state[0::2], state[1::2]):
                top = jnp.maximum(top_a, top_b)
                joined.append(
                    (
                        top,
                        sum_a * jnp.exp(top_a - top) + sum_b * jnp.exp(top_b - top),
                        pick_a + pick_b,
                    )
                )
            state = joined
        top, total, picked = state[0]
        log_total = top + jnp.log(total)
        out_ref[...] = logit_ref[...] - log_total
        draft = picked - log_total
        row = lax.broadcasted_iota(jnp.int32, (rows, LANES), 0)
        lane = lax.broadcasted_iota(jnp.int32, (rows, LANES), 1)
        line = jnp.sum(jnp.where(row == lane, draft, 0.0), axis=0, keepdims=True)
        draft_ref[...] = line[:, 0:rows]

    return pl.pallas_call(
        kernel,
        out_shape=(
            jax.ShapeDtypeStruct((rows, columns), jnp.float32),
            jax.ShapeDtypeStruct((1, rows), jnp.float32),
        ),
        in_specs=[VMEM] * (1 + count),
        out_specs=(VMEM, VMEM),
        compiler_params=params(4),
        cost_estimate=cost(1),
        name="vocab_finish",
    )(resident(logits), *stats)


def pair_sum(array, axis):
    if lax.axis_size(axis) == 2:
        return array, swap(array, axis, 1)
    return lax.psum(array, axis), jnp.zeros_like(array)


def pair_softmax(array, axis, requests, q_width):
    if lax.axis_size(axis) == 2:
        return array, swap(array, axis, 1)
    fold = array.shape[0] // requests
    width = array.shape[1]
    flat = jnp.concatenate(
        [array[i * requests : (i + 1) * requests] for i in range(fold)], axis=1
    )
    every = lax.all_gather(flat, axis)
    tops = every[:, :, q_width : q_width + LANES]
    totals = every[:, :, q_width + LANES :]
    top = jnp.max(tops, axis=0)
    scale = jnp.exp(tops - top)
    heads = q_width // HEAD_DIM
    total = jnp.sum(totals * scale, axis=0)
    mixed = every[:, :, :q_width].reshape(every.shape[0], requests, heads, HEAD_DIM)
    mixed = jnp.sum(mixed * scale[:, :, :heads, None], axis=0).reshape(requests, q_width)
    flat = jnp.concatenate([mixed, top, total], axis=1)
    empty = jnp.concatenate(
        [jnp.zeros_like(mixed), jnp.full_like(top, NEGATIVE), jnp.zeros_like(total)], axis=1
    )

    def folded(value):
        return jnp.concatenate(
            [value[:, i * width : (i + 1) * width] for i in range(fold)], axis=0
        )

    return folded(flat), folded(empty)


def body(
    hidden_in,
    lengths,
    draft_ids,
    input_gain,
    w_query,
    w_latent,
    latent_cache,
    key_up,
    value_up,
    w_out,
    final_gain,
    w_vocab,
):
    rows, depth = hidden_in.shape
    features = depth * lax.axis_size("seq")
    columns = w_vocab.shape[1]
    table = w_vocab.T
    q_width = w_query.shape[1]

    sums = project(
        hidden_in,
        input_gain.reshape(1, depth),
        w_query,
        w_latent.reshape(depth, w_latent.shape[1] * w_latent.shape[2]),
    )
    own, other = pair_sum(sums, "seq")
    cache, keys, values = fetch_attention(
        latent_cache[:, 0], key_up[0], value_up[0], sums, 3
    )
    marks = [0]
    for share in (0.25, 0.55):
        marks.append(int(columns * share) // 512 * 512)
    marks.append(columns)

    packed, local = attend(own, other, lengths, cache, keys, values, features)
    own, other = pair_softmax(packed, "seq", rows, q_width)
    out_table = fetch_rows(w_out, packed, 0, w_out.shape[0], 3)
    part = merge_out(own, other, local, out_table, rows)

    heads = lax.axis_size("heads")
    tables = []
    if is_power(heads) and heads > 1:
        mask = 1
        level = 0
        while True:
            received = swap(part, "heads", mask)
            mask *= 2
            if mask >= heads:
                break
            tables.append(fetch_rows(table, part, marks[level], marks[level + 1], 3))
            level += 1
            part = part + received
    else:
        level = 0
        part, received = lax.psum(part, "heads"), jnp.zeros_like(part)
    tables.append(fetch_rows(table, part, marks[level], columns, 6, 8))

    new_hidden, scaled, square = finish_states(
        part, received, hidden_in, final_gain.reshape(1, depth)
    )
    chunk = round_up(-(-columns // 2), 512)
    bounds = [(0, min(chunk, columns)), (chunk, columns)]
    parts = []
    for first, last in bounds:
        width = round_up(last - first + (LANES if last == columns else 0), 2 * LANES)
        piece = vocab_part(scaled, square, tables, first, last, width)
        parts.append(pair_sum(piece, "seq"))
    logits, stats = vocab_logits(parts, draft_ids, bounds, rows, features)
    if is_power(heads):
        every = [stats] + [swap(stats, "heads", m) for m in range(1, heads)]
    else:
        gathered = lax.all_gather(stats, "heads")
        every = [gathered[i] for i in range(heads)]
        while not is_power(len(every)):
            every.append(jnp.concatenate([jnp.full_like(stats[:, :1], NEGATIVE), jnp.zeros_like(stats[:, 1:])], axis=1))
    log_probs, draft = vocab_finish(logits, every)
    return (new_hidden, log_probs, draft.reshape(rows))


def solution(mesh):
    return jax.shard_map(
        body,
        mesh=mesh,
        in_specs=(
            P("batch", "seq"),
            P("batch"),
            P("batch"),
            P("seq"),
            P("seq", "heads"),
            P("seq", "heads", None),
            P("batch", "heads", "seq", None),
            P("heads", None, None),
            P("heads", None, None),
            P("heads", "seq"),
            P("seq"),
            P("seq", "heads"),
        ),
        out_specs=(P("batch", "seq"), P("batch", "heads"), P("batch")),
        check_vma=False,
    )
```

```python
import math

import jax
import jax.numpy as jnp
from jax import lax
from jax.experimental import pallas as pl
from jax.experimental.pallas import tpu as pltpu
from jax.sharding import PartitionSpec as P


HEAD_DIM = 128
LANES = 128
ROW_TILE = 16
BLOCK = 256
EPSILON = 1e-05
NEGATIVE = -1e30
MIB = 1 << 20
ANY = pl.BlockSpec(memory_space=pl.ANY)
VMEM = pl.BlockSpec(memory_space=pltpu.VMEM)
SMEM = pl.BlockSpec(memory_space=pltpu.SMEM)
NT = (((1,), (1,)), ((), ()))


def resident(array):
    return pltpu.with_memory_space_constraint(array, pltpu.VMEM)


def stored(array):
    return pltpu.with_memory_space_constraint(array, pltpu.HBM)


def cost(micros):
    return pl.CostEstimate(flops=int(micros * 5e6), bytes_accessed=0, transcendentals=0)


def params(mib):
    return pltpu.CompilerParams(vmem_limit_bytes=int(mib * MIB))


def round_up(value, step):
    return -(-value // step) * step


def fold_of(rows, width):
    fold = 8 // math.gcd(rows, 8)
    return fold if width % (fold * LANES) == 0 else 1


def put_folded(ref, rows, start, value):
    width = ref.shape[1]
    done = 0
    while done < value.shape[1]:
        piece, at = divmod(start + done, width)
        size = min(value.shape[1] - done, width - at)
        ref[piece * rows : (piece + 1) * rows, at : at + size] = value[:, done : done + size]
        done += size


def get_folded(refs, rows, start, size):
    width = refs[0].shape[1]
    pieces = []
    done = 0
    while done < size:
        piece, at = divmod(start + done, width)
        span = min(size - done, width - at)
        block = None
        for ref in refs:
            term = ref[piece * rows : (piece + 1) * rows, at : at + span]
            block = term if block is None else block + term
        pieces.append(block)
        done += span
    return pieces[0] if len(pieces) == 1 else jnp.concatenate(pieces, axis=1)


def swap(array, axis, mask):
    size = lax.axis_size(axis)
    return lax.ppermute(array, axis, [(i, i ^ mask) for i in range(size)])


def is_power(size):
    return size & (size - 1) == 0


def project(hidden, gain, w_query, w_latent):
    rows, depth = hidden.shape
    q_width, l_width = w_query.shape[1], w_latent.shape[1]
    width = q_width + l_width + LANES
    fold = fold_of(rows, width)
    chunks = 5 if depth % (5 * LANES) == 0 else 1
    step = depth // chunks

    def kernel(x_hbm, gain_hbm, wq_ref, wl_ref, out_ref, x_ref, gain_ref, q_buf, l_buf, sems, ends):
        small = [
            pltpu.make_async_copy(x_hbm, x_ref, ends.at[0]),
            pltpu.make_async_copy(gain_hbm, gain_ref, ends.at[1]),
        ]
        for copy in small:
            copy.start()
        copies = []
        for c in range(chunks):
            at = pl.ds(c * step, step)
            copies.append(
                (
                    pltpu.make_async_copy(wq_ref.at[at], q_buf.at[at], sems.at[0, c]),
                    pltpu.make_async_copy(wl_ref.at[at], l_buf.at[at], sems.at[1, c]),
                )
            )
        for pair in copies:
            for copy in pair:
                copy.start()
        for copy in small:
            copy.wait()
        states = x_ref[...].astype(jnp.float32)
        gained = (states * gain_ref[...].reshape(1, depth)).astype(jnp.bfloat16)
        square = jnp.sum(states * states, axis=1, keepdims=True)
        acc_q = acc_l = None
        for c in range(chunks):
            for copy in copies[c]:
                copy.wait()
            x = gained[:, c * step : (c + 1) * step]
            part_q = jnp.dot(
                x, q_buf[c * step : (c + 1) * step, :], preferred_element_type=jnp.float32
            )
            part_l = jnp.dot(
                x, l_buf[c * step : (c + 1) * step, :], preferred_element_type=jnp.float32
            )
            acc_q = part_q if c == 0 else acc_q + part_q
            acc_l = part_l if c == 0 else acc_l + part_l
        put_folded(out_ref, rows, 0, acc_q)
        put_folded(out_ref, rows, q_width, acc_l)
        put_folded(out_ref, rows, q_width + l_width, jnp.broadcast_to(square, (rows, LANES)))

    return pl.pallas_call(
        kernel,
        out_shape=jax.ShapeDtypeStruct((rows * fold, width // fold), jnp.float32),
        in_specs=[ANY] * 4,
        out_specs=VMEM,
        scratch_shapes=[
            pltpu.VMEM(hidden.shape, hidden.dtype),
            pltpu.VMEM(gain.shape, gain.dtype),
            pltpu.VMEM(w_query.shape, w_query.dtype),
            pltpu.VMEM(w_latent.shape, w_latent.dtype),
            pltpu.SemaphoreType.DMA((2, chunks)),
            pltpu.SemaphoreType.DMA((2,)),
        ],
        compiler_params=params(14),
        cost_estimate=cost(5),
        name="project",
    )(stored(hidden), stored(gain), stored(w_query), stored(w_latent))


def row_copies(table_ref, out_ref, sems, low, high, step):
    bounds = [(at, min(at + step, high)) for at in range(low, high, step)]
    return [
        pltpu.make_async_copy(
            table_ref.at[pl.ds(a, b - a)], out_ref.at[pl.ds(a - low, b - a)], sems.at[i]
        )
        for i, (a, b) in enumerate(bounds)
    ]


def fetch_turned(table, after, low, high, micros):
    depth = table.shape[1]
    count = high - low

    def kernel(table_ref, after_ref, out_ref, held, sems):
        copies = row_copies(table_ref, held, sems, low, high, BLOCK)
        for copy in copies:
            copy.start()
        for i, copy in enumerate(copies):
            copy.wait()
            a, b = i * BLOCK, min((i + 1) * BLOCK, count)
            for k in range(0, depth, BLOCK):
                end = min(k + BLOCK, depth)
                out_ref[k:end, a:b] = held[a:b, k:end].T

    return pl.pallas_call(
        kernel,
        out_shape=pltpu.VMEM((depth, count), table.dtype),
        in_specs=[ANY, ANY],
        out_specs=VMEM,
        scratch_shapes=[
            pltpu.VMEM((count, depth), table.dtype),
            pltpu.SemaphoreType.DMA((-(-count // BLOCK),)),
        ],
        compiler_params=params(1 + count * round_up(depth, LANES) * 2 / MIB),
        cost_estimate=cost(micros),
        name="fetch_turned",
    )(stored(table), after)


def fetch_attention(cache, key_up, value_up, after, micros):
    rank, width = value_up.shape
    full = round_up(rank, LANES)

    def kernel(cache_ref, key_ref, value_ref, after_ref, cache_out, key_out, value_out, sems):
        copies = [
            pltpu.make_async_copy(key_ref, key_out, sems.at[0]),
            pltpu.make_async_copy(value_ref, value_out.at[pl.ds(full - rank, rank)], sems.at[1]),
            pltpu.make_async_copy(cache_ref, cache_out, sems.at[2]),
        ]
        for copy in copies:
            copy.start()
        value_out[0 : full - rank, :] = jnp.zeros((full - rank, width), value_up.dtype)
        for copy in copies:
            copy.wait()

    return pl.pallas_call(
        kernel,
        out_shape=(
            pltpu.VMEM(cache.shape, cache.dtype),
            pltpu.VMEM(key_up.shape, key_up.dtype),
            pltpu.VMEM((full, width), value_up.dtype),
        ),
        in_specs=[ANY] * 4,
        out_specs=(VMEM,) * 3,
        scratch_shapes=[pltpu.SemaphoreType.DMA((3,))],
        compiler_params=params(1),
        cost_estimate=cost(micros),
        name="fetch_attention",
    )(stored(cache), stored(key_up), stored(value_up), after)


def attend(own, other, lengths, cache, key_up, value_pad, features, w_out, table, low_row, high_row):
    requests, span, width = cache.shape
    rank = width // 2
    full = value_pad.shape[0]
    low = width - full
    heads = key_up.shape[1] // HEAD_DIM
    slot = round_up(heads, 8)
    scaling = 1.0 / math.sqrt(HEAD_DIM)
    q_width = heads * HEAD_DIM
    send_width = q_width + 2 * LANES
    fold = fold_of(requests, send_width)
    tall_step = round_up(-(-(high_row - low_row) // 2), ROW_TILE)

    def kernel(
        own_ref, other_ref, length_ref, cache_ref, key_ref, value_ref, w_ref, table_ref,
        send_ref, local_ref, w_held, table_held, sems, score_own, top_buf, total_buf, latent_buf, stack, *tiles,
    ):
        absorbed, mixed = tiles[: full // LANES], tiles[full // LANES :]
        copies = row_copies(w_ref, w_held, sems.at[0], 0, w_out.shape[0], w_out.shape[0] // 2)
        copies += row_copies(table_ref, table_held, sems.at[1], low_row, high_row, tall_step)
        for copy in copies:
            copy.start()
        refs = (own_ref, other_ref)
        square = get_folded(refs, requests, q_width + width, LANES)
        inv = lax.rsqrt(square[:, 0:1] / features + EPSILON)
        query = (inv * get_folded(refs, requests, 0, q_width)).astype(jnp.bfloat16)
        latent = (inv * get_folded(refs, requests, q_width, width)).astype(jnp.bfloat16)
        latent_buf[...] = latent.astype(jnp.float32)
        for tile in absorbed:
            tile[...] = jnp.zeros(tile.shape, jnp.float32)
        for j in range(heads):
            at = slice(j * HEAD_DIM, (j + 1) * HEAD_DIM)
            row = lax.dot_general(
                query[:, at], key_ref[:, at], NT, preferred_element_type=jnp.float32
            )
            row = row.astype(jnp.bfloat16).astype(jnp.float32)
            for i, tile in enumerate(absorbed):
                piece = row[:, i * LANES : min((i + 1) * LANES, rank)]
                if piece.shape[1] < LANES:
                    edge = jnp.zeros((requests, LANES - piece.shape[1]), jnp.float32)
                    piece = jnp.concatenate([piece, edge], axis=1)
                tile[pl.ds(j, requests, stride=slot), :] = piece
        first = lax.axis_index("seq") * span
        positions = first + lax.broadcasted_iota(jnp.int32, (slot, span), 1)
        for b in range(requests):
            at = slice(b * slot, (b + 1) * slot)
            rows = jnp.concatenate([tile[at, :] for tile in absorbed], axis=1)
            score_own[at, :] = jnp.broadcast_to(
                jnp.sum(rows * latent_buf[b : b + 1, 0:full], axis=1, keepdims=True) * scaling,
                (slot, LANES),
            )
            scores = (
                lax.dot_general(
                    rows.astype(jnp.bfloat16),
                    cache_ref[b, :, 0:full],
                    NT,
                    preferred_element_type=jnp.float32,
                )
                * scaling
            )
            live = positions < length_ref[b]
            scores = jnp.where(live, scores, NEGATIVE)
            top = jnp.max(scores, axis=1, keepdims=True)
            weights = jnp.where(live, jnp.exp(scores - top), 0.0)
            top_buf[at, :] = jnp.broadcast_to(top, (slot, LANES))
            total_buf[at, :] = jnp.broadcast_to(
                jnp.sum(weights, axis=1, keepdims=True), (slot, LANES)
            )
            value = jnp.dot(
                weights.astype(jnp.bfloat16),
                cache_ref[b, :, low:width],
                preferred_element_type=jnp.float32,
            )
            for i, tile in enumerate(mixed):
                tile[at, :] = value[:, i * LANES : (i + 1) * LANES]
        lane = lax.broadcasted_iota(jnp.int32, (requests, LANES), 1)
        tops = jnp.full((requests, LANES), NEGATIVE, jnp.float32)
        owns = jnp.full((requests, LANES), NEGATIVE, jnp.float32)
        totals = jnp.zeros((requests, LANES), jnp.float32)
        second = ROW_TILE * -(-requests // ROW_TILE)
        stack[2 * second : 2 * second + requests, :] = latent[:, low:width]
        for j in range(heads):
            pick = pl.ds(j, requests, stride=slot)
            tops = jnp.where(lane == j, top_buf[pick, :], tops)
            totals = jnp.where(lane == j, total_buf[pick, :], totals)
            owns = jnp.where(lane == j, score_own[pick, :], owns)
            value = jnp.concatenate([tile[pick, :] for tile in mixed], axis=1)
            high = value.astype(jnp.bfloat16)
            stack[0:requests, :] = high
            stack[second : second + requests, :] = (value - high.astype(jnp.float32)).astype(
                jnp.bfloat16
            )
            at = slice(j * HEAD_DIM, (j + 1) * HEAD_DIM)
            lifted = jnp.dot(stack[...], value_ref[:, at], preferred_element_type=jnp.float32)
            put_folded(
                send_ref, requests, j * HEAD_DIM,
                lifted[0:requests] + lifted[second : second + requests],
            )
            local_ref[:, at] = lifted[2 * second : 2 * second + requests]
        put_folded(send_ref, requests, q_width, tops)
        put_folded(send_ref, requests, q_width + LANES, totals)
        local_ref[:, q_width : q_width + LANES] = owns
        for copy in copies:
            copy.wait()

    tall = requests * slot
    return pl.pallas_call(
        kernel,
        out_shape=(
            jax.ShapeDtypeStruct((requests * fold, send_width // fold), jnp.float32),
            jax.ShapeDtypeStruct((requests, q_width + LANES), jnp.float32),
            pltpu.VMEM(w_out.shape, w_out.dtype),
            pltpu.VMEM((high_row - low_row, table.shape[1]), table.dtype),
        ),
        in_specs=[VMEM, VMEM, SMEM, VMEM, VMEM, VMEM, ANY, ANY],
        out_specs=(VMEM,) * 4,
        scratch_shapes=[
            pltpu.SemaphoreType.DMA((2, 2)),
            pltpu.VMEM((tall, LANES), jnp.float32),
            pltpu.VMEM((tall, LANES), jnp.float32),
            pltpu.VMEM((tall, LANES), jnp.float32),
            pltpu.VMEM((requests, width), jnp.float32),
            pltpu.VMEM((3 * round_up(requests, ROW_TILE), full), jnp.bfloat16),
        ]
        + [pltpu.VMEM((tall, LANES), jnp.float32)] * (2 * full // LANES),
        compiler_params=params(5),
        cost_estimate=cost(5),
        name="attend",
    )(
        own, other, lengths, resident(cache), resident(key_up), resident(value_pad),
        stored(w_out), stored(table),
    )


def merge_out(own, other, local, w_out, requests):
    q_width = local.shape[1] - LANES
    heads = q_width // HEAD_DIM
    width = w_out.shape[1]
    fold = fold_of(requests, width)
    step = 512 if width % 512 == 0 else width

    def kernel(own_ref, other_ref, local_ref, w_ref, out_ref, head_buf):
        top_a = get_folded((own_ref,), requests, q_width, LANES)
        top_b = get_folded((other_ref,), requests, q_width, LANES)
        total_a = get_folded((own_ref,), requests, q_width + LANES, LANES)
        total_b = get_folded((other_ref,), requests, q_width + LANES, LANES)
        own_score = local_ref[:, q_width : q_width + LANES]
        highest = jnp.maximum(jnp.maximum(top_a, top_b), own_score)
        scale_a = jnp.exp(top_a - highest)
        scale_b = jnp.exp(top_b - highest)
        own_weight = jnp.exp(own_score - highest)
        below = total_a * scale_a + total_b * scale_b + own_weight
        scale_a = scale_a / below
        scale_b = scale_b / below
        own_weight = own_weight / below
        for j in range(heads):
            at = slice(j * HEAD_DIM, (j + 1) * HEAD_DIM)
            value = (
                get_folded((own_ref,), requests, j * HEAD_DIM, HEAD_DIM) * scale_a[:, j : j + 1]
                + get_folded((other_ref,), requests, j * HEAD_DIM, HEAD_DIM)
                * scale_b[:, j : j + 1]
                + local_ref[:, at] * own_weight[:, j : j + 1]
            )
            head_buf[:, at] = value.astype(jnp.bfloat16)
        head_out = head_buf[...]
        for at in range(0, width, step):
            put_folded(
                out_ref, requests, at,
                jnp.dot(head_out, w_ref[:, at : at + step], preferred_element_type=jnp.float32),
            )

    return pl.pallas_call(
        kernel,
        out_shape=jax.ShapeDtypeStruct((requests * fold, width // fold), jnp.float32),
        in_specs=[VMEM] * 4,
        out_specs=VMEM,
        scratch_shapes=[pltpu.VMEM((requests, q_width), jnp.bfloat16)],
        compiler_params=params(3),
        cost_estimate=cost(2),
        name="merge_out",
    )(own, other, local, resident(w_out))


def put_terms(out_ref, rows, start, x, table_ref, turned):
    count = table_ref.shape[1] if turned else table_ref.shape[0]
    depth = x.shape[1]
    half = depth // 2 if depth % (2 * LANES) == 0 else depth
    for at in range(0, count, 2 * BLOCK):
        end = min(at + 2 * BLOCK, count)
        total = None
        for k in range(0, depth, half):
            piece = x[:, k : k + half]
            if turned:
                term = jnp.dot(
                    piece, table_ref[k : k + half, at:end], preferred_element_type=jnp.float32
                )
            else:
                term = lax.dot_general(
                    piece, table_ref[at:end, k : k + half], NT, preferred_element_type=jnp.float32
                )
            total = term if total is None else total + term
        put_folded(out_ref, rows, start + at, total)


def vocab_head(own, other, hidden, gain, turned, table, low_row, high_row, width):
    rows, depth = hidden.shape
    fold = fold_of(rows, width)
    count = len(turned)
    pieces = 4
    step = round_up(-(-(high_row - low_row) // pieces), ROW_TILE)

    def kernel(own_ref, other_ref, x_ref, gain_ref, *refs):
        table_ref = refs[count]
        new_ref, scaled_ref, square_ref, out_ref, held, sems = refs[count + 1 :]
        copies = row_copies(table_ref, held, sems, low_row, high_row, step)
        for copy in copies:
            copy.start()
        states = x_ref[...].astype(jnp.float32)
        updated = states + get_folded((own_ref, other_ref), rows, 0, depth)
        new_ref[...] = updated.astype(jnp.bfloat16)
        scaled = (updated * gain_ref[...].reshape(1, depth)).astype(jnp.bfloat16)
        scaled_ref[...] = scaled
        square_ref[...] = jnp.broadcast_to(
            jnp.sum(updated * updated, axis=1, keepdims=True), (rows, LANES)
        )
        start = 0
        for turned_ref in refs[:count]:
            put_terms(out_ref, rows, start, scaled, turned_ref, True)
            start += turned_ref.shape[1]
        for copy in copies:
            copy.wait()

    return pl.pallas_call(
        kernel,
        out_shape=(
            jax.ShapeDtypeStruct((rows, depth), jnp.bfloat16),
            jax.ShapeDtypeStruct((rows, depth), jnp.bfloat16),
            jax.ShapeDtypeStruct((rows, LANES), jnp.float32),
            jax.ShapeDtypeStruct((rows * fold, width // fold), jnp.float32),
            pltpu.VMEM((high_row - low_row, depth), table.dtype),
        ),
        in_specs=[VMEM] * (4 + count) + [ANY],
        out_specs=(VMEM,) * 5,
        scratch_shapes=[pltpu.SemaphoreType.DMA((pieces,))],
        compiler_params=params(3),
        cost_estimate=cost(4),
        name="vocab_head",
    )(own, other, hidden, gain, *[resident(part) for part in turned], stored(table))


def vocab_tail(scaled, square, tables, width):
    rows = scaled.shape[0]
    fold = fold_of(rows, width)
    used = sum(table.shape[0] for table in tables)

    def kernel(x_ref, square_ref, *refs):
        out_ref = refs[-1]
        x = x_ref[...]
        start = 0
        for table_ref in refs[:-1]:
            put_terms(out_ref, rows, start, x, table_ref, False)
            start += table_ref.shape[0]
        put_folded(
            out_ref, rows, used,
            jnp.broadcast_to(square_ref[:, 0:1], (rows, width - used)),
        )

    return pl.pallas_call(
        kernel,
        out_shape=jax.ShapeDtypeStruct((rows * fold, width // fold), jnp.float32),
        in_specs=[VMEM] * (2 + len(tables)),
        out_specs=VMEM,
        compiler_params=params(3),
        cost_estimate=cost(6),
        name="vocab_tail",
    )(scaled, square, *[resident(table) for table in tables])


def vocab_logits(parts, draft_ids, bounds, rows, features):
    columns = bounds[-1][1]
    count = len(bounds)
    flat = [array for pair in parts for array in pair]

    def kernel(id_ref, *refs):
        pairs = [refs[2 * i : 2 * i + 2] for i in range(count)]
        logit_ref, stat_ref = refs[2 * count :]
        full = pairs[-1][0].shape[0] * pairs[-1][0].shape[1] // rows
        square = get_folded(pairs[-1], rows, full - LANES, LANES)
        inv = lax.rsqrt(square[:, 0:1] / features + EPSILON)
        row = lax.broadcasted_iota(jnp.int32, (rows, 1), 0)
        wanted = jnp.zeros((rows, 1), jnp.int32)
        for r in range(rows):
            wanted = jnp.where(row == r, id_ref[r], wanted)
        wanted = wanted - lax.axis_index("heads") * columns
        top = jnp.full((rows, 1), NEGATIVE, jnp.float32)
        picked = jnp.zeros((rows, 1), jnp.float32)
        for pair, (first, last) in zip(pairs, bounds):
            logits = get_folded(pair, rows, 0, last - first) * inv
            logit_ref[:, first:last] = logits
            top = jnp.maximum(top, jnp.max(logits, axis=1, keepdims=True))
            column = first + lax.broadcasted_iota(jnp.int32, logits.shape, 1)
            picked = picked + jnp.sum(
                jnp.where(column == wanted, logits, 0.0), axis=1, keepdims=True
            )
        total = jnp.zeros((rows, 1), jnp.float32)
        for first, last in bounds:
            total = total + jnp.sum(
                jnp.exp(logit_ref[:, first:last] - top), axis=1, keepdims=True
            )
        lane = lax.broadcasted_iota(jnp.int32, (rows, LANES), 1)
        stat_ref[...] = jnp.where(
            lane == 0, top, jnp.where(lane == 1, total, jnp.where(lane == 2, picked, 0.0))
        )

    return pl.pallas_call(
        kernel,
        out_shape=(
            pltpu.VMEM((rows, columns), jnp.float32),
            jax.ShapeDtypeStruct((rows, LANES), jnp.float32),
        ),
        in_specs=[SMEM] + [VMEM] * len(flat),
        out_specs=(VMEM, VMEM),
        compiler_params=params(4),
        cost_estimate=cost(2),
        name="vocab_logits",
    )(draft_ids, *flat)


def vocab_finish(logits, stats):
    rows, columns = logits.shape
    count = len(stats)

    def kernel(logit_ref, *refs):
        stat_refs, out_ref, draft_ref = refs[:count], refs[count], refs[count + 1]
        state = [(ref[:, 0:1], ref[:, 1:2], ref[:, 2:3]) for ref in stat_refs]
        while len(state) > 1:
            joined = []
            for (top_a, sum_a, pick_a), (top_b, sum_b, pick_b) in zip(state[0::2], state[1::2]):
                top = jnp.maximum(top_a, top_b)
                joined.append(
                    (
                        top,
                        sum_a * jnp.exp(top_a - top) + sum_b * jnp.exp(top_b - top),
                        pick_a + pick_b,
                    )
                )
            state = joined
        top, total, picked = state[0]
        log_total = top + jnp.log(total)
        out_ref[...] = logit_ref[...] - log_total
        draft = picked - log_total
        row = lax.broadcasted_iota(jnp.int32, (rows, LANES), 0)
        lane = lax.broadcasted_iota(jnp.int32, (rows, LANES), 1)
        line = jnp.sum(jnp.where(row == lane, draft, 0.0), axis=0, keepdims=True)
        draft_ref[...] = line[:, 0:rows]

    return pl.pallas_call(
        kernel,
        out_shape=(
            jax.ShapeDtypeStruct((rows, columns), jnp.float32),
            jax.ShapeDtypeStruct((1, rows), jnp.float32),
        ),
        in_specs=[VMEM] * (1 + count),
        out_specs=(VMEM, VMEM),
        compiler_params=params(4),
        cost_estimate=cost(1),
        name="vocab_finish",
    )(resident(logits), *stats)


def pair_sum(array, axis):
    if lax.axis_size(axis) == 2:
        return array, swap(array, axis, 1)
    return lax.psum(array, axis), jnp.zeros_like(array)


def pair_softmax(array, axis, requests, q_width):
    if lax.axis_size(axis) == 2:
        return array, swap(array, axis, 1)
    fold = array.shape[0] // requests
    width = array.shape[1]
    flat = jnp.concatenate(
        [array[i * requests : (i + 1) * requests] for i in range(fold)], axis=1
    )
    every = lax.all_gather(flat, axis)
    tops = every[:, :, q_width : q_width + LANES]
    totals = every[:, :, q_width + LANES :]
    top = jnp.max(tops, axis=0)
    scale = jnp.exp(tops - top)
    heads = q_width // HEAD_DIM
    total = jnp.sum(totals * scale, axis=0)
    mixed = every[:, :, :q_width].reshape(every.shape[0], requests, heads, HEAD_DIM)
    mixed = jnp.sum(mixed * scale[:, :, :heads, None], axis=0).reshape(requests, q_width)
    flat = jnp.concatenate([mixed, top, total], axis=1)
    empty = jnp.concatenate(
        [jnp.zeros_like(mixed), jnp.full_like(top, NEGATIVE), jnp.zeros_like(total)], axis=1
    )

    def folded(value):
        return jnp.concatenate(
            [value[:, i * width : (i + 1) * width] for i in range(fold)], axis=0
        )

    return folded(flat), folded(empty)


def body(
    hidden_in,
    lengths,
    draft_ids,
    input_gain,
    w_query,
    w_latent,
    latent_cache,
    key_up,
    value_up,
    w_out,
    final_gain,
    w_vocab,
):
    rows, depth = hidden_in.shape
    features = depth * lax.axis_size("seq")
    columns = w_vocab.shape[1]
    table = w_vocab.T
    q_width = w_query.shape[1]

    def mark(share):
        return int(columns * share) // BLOCK * BLOCK

    marks = [0, mark(0.16), mark(0.336), mark(0.64), mark(0.82), columns]

    sums = project(
        hidden_in,
        input_gain,
        w_query,
        w_latent.reshape(depth, w_latent.shape[1] * w_latent.shape[2]),
    )
    own, other = pair_sum(sums, "seq")
    cache, keys, values = fetch_attention(
        latent_cache[:, 0], key_up[0], value_up[0], sums, 3
    )
    packed, local, out_table, stored_part = attend(
        own, other, lengths, cache, keys, values, features, w_out, table, marks[3], marks[4]
    )
    own, other = pair_softmax(packed, "seq", rows, q_width)
    turned = [fetch_turned(table, packed, marks[0], marks[1], 3)]
    part = merge_out(own, other, local, out_table, rows)

    heads = lax.axis_size("heads")
    first = part
    if is_power(heads) and heads > 1:
        mask = 1
        while True:
            received = swap(part, "heads", mask)
            mask *= 2
            if mask >= heads:
                break
            part = part + received
    else:
        part, received = lax.psum(part, "heads"), jnp.zeros_like(part)
    turned.append(fetch_turned(table, first, marks[1], marks[2], 3))
    turned.append(fetch_turned(table, part, marks[2], marks[3], 6))

    bounds = [(0, marks[3]), (marks[3], columns)]
    tail_width = round_up(columns - marks[3] + LANES, 2 * LANES)
    new_hidden, scaled, square, piece, late_part = vocab_head(
        part, received, hidden_in, final_gain, turned, table, marks[4], columns, marks[3]
    )
    parts = [pair_sum(piece, "seq")]
    piece = vocab_tail(scaled, square, [stored_part, late_part], tail_width)
    parts.append(pair_sum(piece, "seq"))
    logits, stats = vocab_logits(parts, draft_ids, bounds, rows, features)
    if is_power(heads):
        every = [stats] + [swap(stats, "heads", m) for m in range(1, heads)]
    else:
        gathered = lax.all_gather(stats, "heads")
        every = [gathered[i] for i in range(heads)]
        while not is_power(len(every)):
            every.append(jnp.concatenate([jnp.full_like(stats[:, :1], NEGATIVE), jnp.zeros_like(stats[:, 1:])], axis=1))
    log_probs, draft = vocab_finish(logits, every)
    return (new_hidden, log_probs, draft.reshape(rows))


def solution(mesh):
    return jax.shard_map(
        body,
        mesh=mesh,
        in_specs=(
            P("batch", "seq"),
            P("batch"),
            P("batch"),
            P("seq"),
            P("seq", "heads"),
            P("seq", "heads", None),
            P("batch", "heads", "seq", None),
            P("heads", None, None),
            P("heads", None, None),
            P("heads", "seq"),
            P("seq"),
            P("seq", "heads"),
        ),
        out_specs=(P("batch", "seq"), P("batch", "heads"), P("batch")),
        check_vma=False,
    )
```

```python
import math

import jax
import jax.numpy as jnp
from jax import lax
from jax.experimental import pallas as pl
from jax.experimental.pallas import tpu as pltpu
from jax.sharding import PartitionSpec as P


HEAD_DIM = 128
LANES = 128
ROW_TILE = 16
BLOCK = 256
EPSILON = 1e-05
NEGATIVE = -1e30
MIB = 1 << 20
ANY = pl.BlockSpec(memory_space=pl.ANY)
VMEM = pl.BlockSpec(memory_space=pltpu.VMEM)
SMEM = pl.BlockSpec(memory_space=pltpu.SMEM)
NT = (((1,), (1,)), ((), ()))


def resident(array):
    return pltpu.with_memory_space_constraint(array, pltpu.VMEM)


def stored(array):
    return pltpu.with_memory_space_constraint(array, pltpu.HBM)


def cost(micros):
    return pl.CostEstimate(flops=int(micros * 5e6), bytes_accessed=0, transcendentals=0)


def params(mib):
    return pltpu.CompilerParams(vmem_limit_bytes=int(mib * MIB))


def round_up(value, step):
    return -(-value // step) * step


def fold_of(rows, width):
    fold = 8 // math.gcd(rows, 8)
    return fold if width % (fold * LANES) == 0 else 1


def put_folded(ref, rows, start, value):
    width = ref.shape[1]
    done = 0
    while done < value.shape[1]:
        piece, at = divmod(start + done, width)
        size = min(value.shape[1] - done, width - at)
        ref[piece * rows : (piece + 1) * rows, at : at + size] = value[:, done : done + size]
        done += size


def get_folded(refs, rows, start, size):
    width = refs[0].shape[1]
    pieces = []
    done = 0
    while done < size:
        piece, at = divmod(start + done, width)
        span = min(size - done, width - at)
        block = None
        for ref in refs:
            term = ref[piece * rows : (piece + 1) * rows, at : at + span]
            block = term if block is None else block + term
        pieces.append(block)
        done += span
    return pieces[0] if len(pieces) == 1 else jnp.concatenate(pieces, axis=1)


def swap(array, axis, mask):
    size = lax.axis_size(axis)
    return lax.ppermute(array, axis, [(i, i ^ mask) for i in range(size)])


def fence(sem):
    pl.semaphore_signal(sem, 1)
    pl.semaphore_wait(sem, 1)


def is_power(size):
    return size & (size - 1) == 0


def project(hidden, gain, w_query, w_latent):
    rows, depth = hidden.shape
    q_width, l_width = w_query.shape[1], w_latent.shape[1]
    width = q_width + l_width + LANES
    fold = fold_of(rows, width)
    chunks = 5 if depth % (5 * LANES) == 0 else 1
    step = depth // chunks

    def kernel(x_hbm, gain_hbm, wq_ref, wl_ref, out_ref, x_ref, gain_ref, q_buf, l_buf, sems, ends, gate):
        small = [
            pltpu.make_async_copy(x_hbm, x_ref, ends.at[0]),
            pltpu.make_async_copy(gain_hbm, gain_ref, ends.at[1]),
        ]
        for copy in small:
            copy.start()
        fence(gate)
        copies = []
        for c in range(chunks):
            at = pl.ds(c * step, step)
            copies.append(
                (
                    pltpu.make_async_copy(wq_ref.at[at], q_buf.at[at], sems.at[0, c]),
                    pltpu.make_async_copy(wl_ref.at[at], l_buf.at[at], sems.at[1, c]),
                )
            )
        for pair in copies:
            for copy in pair:
                copy.start()
        for copy in small:
            copy.wait()
        states = x_ref[...].astype(jnp.float32)
        gained = (states * gain_ref[...].reshape(1, depth)).astype(jnp.bfloat16)
        square = jnp.sum(states * states, axis=1, keepdims=True)
        acc_q = acc_l = None
        for c in range(chunks):
            for copy in copies[c]:
                copy.wait()
            x = gained[:, c * step : (c + 1) * step]
            part_q = jnp.dot(
                x, q_buf[c * step : (c + 1) * step, :], preferred_element_type=jnp.float32
            )
            part_l = jnp.dot(
                x, l_buf[c * step : (c + 1) * step, :], preferred_element_type=jnp.float32
            )
            acc_q = part_q if c == 0 else acc_q + part_q
            acc_l = part_l if c == 0 else acc_l + part_l
        put_folded(out_ref, rows, 0, acc_q)
        put_folded(out_ref, rows, q_width, acc_l)
        put_folded(out_ref, rows, q_width + l_width, jnp.broadcast_to(square, (rows, LANES)))

    return pl.pallas_call(
        kernel,
        out_shape=jax.ShapeDtypeStruct((rows * fold, width // fold), jnp.float32),
        in_specs=[ANY] * 4,
        out_specs=VMEM,
        scratch_shapes=[
            pltpu.VMEM(hidden.shape, hidden.dtype),
            pltpu.VMEM(gain.shape, gain.dtype),
            pltpu.VMEM(w_query.shape, w_query.dtype),
            pltpu.VMEM(w_latent.shape, w_latent.dtype),
            pltpu.SemaphoreType.DMA((2, chunks)),
            pltpu.SemaphoreType.DMA((2,)),
            pltpu.SemaphoreType.REGULAR,
        ],
        compiler_params=params(14),
        cost_estimate=cost(5),
        name="project",
    )(stored(hidden), stored(gain), stored(w_query), stored(w_latent))


def row_copies(table_ref, out_ref, sems, low, high, step):
    bounds = [(at, min(at + step, high)) for at in range(low, high, step)]
    return [
        pltpu.make_async_copy(
            table_ref.at[pl.ds(a, b - a)], out_ref.at[pl.ds(a - low, b - a)], sems.at[i]
        )
        for i, (a, b) in enumerate(bounds)
    ]


def fetch_turned(table, after, low, high, micros):
    depth = table.shape[1]
    count = high - low

    def kernel(table_ref, after_ref, out_ref, held, sems):
        copies = row_copies(table_ref, held, sems, low, high, BLOCK)
        for copy in copies:
            copy.start()
        for i, copy in enumerate(copies):
            copy.wait()
            a, b = i * BLOCK, min((i + 1) * BLOCK, count)
            for k in range(0, depth, BLOCK):
                end = min(k + BLOCK, depth)
                out_ref[k:end, a:b] = held[a:b, k:end].T

    return pl.pallas_call(
        kernel,
        out_shape=pltpu.VMEM((depth, count), table.dtype),
        in_specs=[ANY, ANY],
        out_specs=VMEM,
        scratch_shapes=[
            pltpu.VMEM((count, depth), table.dtype),
            pltpu.SemaphoreType.DMA((-(-count // BLOCK),)),
        ],
        compiler_params=params(1 + count * round_up(depth, LANES) * 2 / MIB),
        cost_estimate=cost(micros),
        name="fetch_turned",
    )(stored(table), after)


def fetch_attention(cache, key_up, value_up, after, micros):
    rank, width = value_up.shape
    full = round_up(rank, LANES)

    def kernel(cache_ref, key_ref, value_ref, after_ref, cache_out, key_out, value_out, sems):
        copies = [
            pltpu.make_async_copy(key_ref, key_out, sems.at[0]),
            pltpu.make_async_copy(value_ref, value_out.at[pl.ds(full - rank, rank)], sems.at[1]),
            pltpu.make_async_copy(cache_ref, cache_out, sems.at[2]),
        ]
        for copy in copies:
            copy.start()
        value_out[0 : full - rank, :] = jnp.zeros((full - rank, width), value_up.dtype)
        for copy in copies:
            copy.wait()

    return pl.pallas_call(
        kernel,
        out_shape=(
            pltpu.VMEM(cache.shape, cache.dtype),
            pltpu.VMEM(key_up.shape, key_up.dtype),
            pltpu.VMEM((full, width), value_up.dtype),
        ),
        in_specs=[ANY] * 4,
        out_specs=(VMEM,) * 3,
        scratch_shapes=[pltpu.SemaphoreType.DMA((3,))],
        compiler_params=params(1),
        cost_estimate=cost(micros),
        name="fetch_attention",
    )(stored(cache), stored(key_up), stored(value_up), after)


def attend(own, other, lengths, cache, key_up, value_pad, features, w_out):
    requests, span, width = cache.shape
    rank = width // 2
    full = value_pad.shape[0]
    low = width - full
    heads = key_up.shape[1] // HEAD_DIM
    slot = round_up(heads, ROW_TILE)
    scaling = 1.0 / math.sqrt(HEAD_DIM)
    q_width = heads * HEAD_DIM
    send_width = q_width + 2 * LANES
    fold = fold_of(requests, send_width)

    def kernel(
        own_ref, other_ref, length_ref, cache_ref, key_ref, value_ref, w_ref,
        send_ref, local_ref, w_held, sems, gate, score_own, top_buf, total_buf, latent_buf, stack,
        score_buf, weight_buf, *tiles,
    ):
        absorbed, mixed = tiles[: full // LANES], tiles[full // LANES :]
        copies = row_copies(w_ref, w_held, sems, 0, w_out.shape[0], w_out.shape[0] // 2)
        for copy in copies:
            copy.start()
        fence(gate)
        refs = (own_ref, other_ref)
        square = get_folded(refs, requests, q_width + width, LANES)
        inv = lax.rsqrt(square[:, 0:1] / features + EPSILON)
        query = (inv * get_folded(refs, requests, 0, q_width)).astype(jnp.bfloat16)
        latent = (inv * get_folded(refs, requests, q_width, width)).astype(jnp.bfloat16)
        latent_buf[...] = latent.astype(jnp.float32)
        for tile in absorbed:
            tile[...] = jnp.zeros(tile.shape, jnp.float32)
        for j in range(heads):
            at = slice(j * HEAD_DIM, (j + 1) * HEAD_DIM)
            row = lax.dot_general(
                query[:, at], key_ref[:, at], NT, preferred_element_type=jnp.float32
            )
            row = row.astype(jnp.bfloat16).astype(jnp.float32)
            for i, tile in enumerate(absorbed):
                piece = row[:, i * LANES : min((i + 1) * LANES, rank)]
                if piece.shape[1] < LANES:
                    edge = jnp.zeros((requests, LANES - piece.shape[1]), jnp.float32)
                    piece = jnp.concatenate([piece, edge], axis=1)
                tile[pl.ds(j, requests, stride=slot), :] = piece
        first = lax.axis_index("seq") * span
        positions = first + lax.broadcasted_iota(jnp.int32, (slot, span), 1)
        spans = [slice(b * slot, (b + 1) * slot) for b in range(requests)]
        for b, at in enumerate(spans):
            rows = jnp.concatenate([tile[at, :] for tile in absorbed], axis=1)
            score_buf[at, :] = lax.dot_general(
                rows.astype(jnp.bfloat16),
                cache_ref[b, :, 0:full],
                NT,
                preferred_element_type=jnp.float32,
            )
            score_own[at, :] = jnp.broadcast_to(
                jnp.sum(rows * latent_buf[b : b + 1, 0:full], axis=1, keepdims=True) * scaling,
                (slot, LANES),
            )
        for b, at in enumerate(spans):
            live = positions < length_ref[b]
            scores = jnp.where(live, score_buf[at, :] * scaling, NEGATIVE)
            top = jnp.max(scores, axis=1, keepdims=True)
            weights = jnp.where(live, jnp.exp(scores - top), 0.0)
            top_buf[at, :] = jnp.broadcast_to(top, (slot, LANES))
            total_buf[at, :] = jnp.broadcast_to(
                jnp.sum(weights, axis=1, keepdims=True), (slot, LANES)
            )
            weight_buf[at, :] = weights.astype(jnp.bfloat16)
        for b, at in enumerate(spans):
            value = jnp.dot(
                weight_buf[at, :], cache_ref[b, :, low:width], preferred_element_type=jnp.float32
            )
            for i, tile in enumerate(mixed):
                tile[at, :] = value[:, i * LANES : (i + 1) * LANES]
        lane = lax.broadcasted_iota(jnp.int32, (requests, LANES), 1)
        tops = jnp.full((requests, LANES), NEGATIVE, jnp.float32)
        owns = jnp.full((requests, LANES), NEGATIVE, jnp.float32)
        totals = jnp.zeros((requests, LANES), jnp.float32)
        second = ROW_TILE * -(-requests // ROW_TILE)
        stack[2 * second : 2 * second + requests, :] = latent[:, low:width]
        for j in range(heads):
            pick = pl.ds(j, requests, stride=slot)
            tops = jnp.where(lane == j, top_buf[pick, :], tops)
            totals = jnp.where(lane == j, total_buf[pick, :], totals)
            owns = jnp.where(lane == j, score_own[pick, :], owns)
            value = jnp.concatenate([tile[pick, :] for tile in mixed], axis=1)
            high = value.astype(jnp.bfloat16)
            stack[0:requests, :] = high
            stack[second : second + requests, :] = (value - high.astype(jnp.float32)).astype(
                jnp.bfloat16
            )
            at = slice(j * HEAD_DIM, (j + 1) * HEAD_DIM)
            lifted = jnp.dot(stack[...], value_ref[:, at], preferred_element_type=jnp.float32)
            put_folded(
                send_ref, requests, j * HEAD_DIM,
                lifted[0:requests] + lifted[second : second + requests],
            )
            local_ref[:, at] = lifted[2 * second : 2 * second + requests]
        put_folded(send_ref, requests, q_width, tops)
        put_folded(send_ref, requests, q_width + LANES, totals)
        local_ref[:, q_width : q_width + LANES] = owns
        for copy in copies:
            copy.wait()

    tall = requests * slot
    return pl.pallas_call(
        kernel,
        out_shape=(
            jax.ShapeDtypeStruct((requests * fold, send_width // fold), jnp.float32),
            jax.ShapeDtypeStruct((requests, q_width + LANES), jnp.float32),
            pltpu.VMEM(w_out.shape, w_out.dtype),
        ),
        in_specs=[VMEM, VMEM, SMEM, VMEM, VMEM, VMEM, ANY],
        out_specs=(VMEM,) * 3,
        scratch_shapes=[
            pltpu.SemaphoreType.DMA((2,)),
            pltpu.SemaphoreType.REGULAR,
            pltpu.VMEM((tall, LANES), jnp.float32),
            pltpu.VMEM((tall, LANES), jnp.float32),
            pltpu.VMEM((tall, LANES), jnp.float32),
            pltpu.VMEM((requests, width), jnp.float32),
            pltpu.VMEM((3 * round_up(requests, ROW_TILE), full), jnp.bfloat16),
            pltpu.VMEM((tall, span), jnp.float32),
            pltpu.VMEM((tall, span), jnp.bfloat16),
        ]
        + [pltpu.VMEM((tall, LANES), jnp.float32)] * (2 * full // LANES),
        compiler_params=params(5),
        cost_estimate=cost(5),
        name="attend",
    )(
        own, other, lengths, resident(cache), resident(key_up), resident(value_pad),
        stored(w_out),
    )


def merge_out(own, other, local, w_out, requests):
    q_width = local.shape[1] - LANES
    heads = q_width // HEAD_DIM
    width = w_out.shape[1]
    fold = fold_of(requests, width)
    step = 512 if width % 512 == 0 else width

    def kernel(own_ref, other_ref, local_ref, w_ref, out_ref, head_buf):
        top_a = get_folded((own_ref,), requests, q_width, LANES)
        top_b = get_folded((other_ref,), requests, q_width, LANES)
        total_a = get_folded((own_ref,), requests, q_width + LANES, LANES)
        total_b = get_folded((other_ref,), requests, q_width + LANES, LANES)
        own_score = local_ref[:, q_width : q_width + LANES]
        highest = jnp.maximum(jnp.maximum(top_a, top_b), own_score)
        scale_a = jnp.exp(top_a - highest)
        scale_b = jnp.exp(top_b - highest)
        own_weight = jnp.exp(own_score - highest)
        below = total_a * scale_a + total_b * scale_b + own_weight
        scale_a = scale_a / below
        scale_b = scale_b / below
        own_weight = own_weight / below
        for j in range(heads):
            at = slice(j * HEAD_DIM, (j + 1) * HEAD_DIM)
            value = (
                get_folded((own_ref,), requests, j * HEAD_DIM, HEAD_DIM) * scale_a[:, j : j + 1]
                + get_folded((other_ref,), requests, j * HEAD_DIM, HEAD_DIM)
                * scale_b[:, j : j + 1]
                + local_ref[:, at] * own_weight[:, j : j + 1]
            )
            head_buf[:, at] = value.astype(jnp.bfloat16)
        head_out = head_buf[...]
        for at in range(0, width, step):
            put_folded(
                out_ref, requests, at,
                jnp.dot(head_out, w_ref[:, at : at + step], preferred_element_type=jnp.float32),
            )

    return pl.pallas_call(
        kernel,
        out_shape=jax.ShapeDtypeStruct((requests * fold, width // fold), jnp.float32),
        in_specs=[VMEM] * 4,
        out_specs=VMEM,
        scratch_shapes=[pltpu.VMEM((requests, q_width), jnp.bfloat16)],
        compiler_params=params(3),
        cost_estimate=cost(2),
        name="merge_out",
    )(own, other, local, resident(w_out))


def put_terms(out_ref, rows, start, x, table_ref, turned):
    count = table_ref.shape[1] if turned else table_ref.shape[0]
    depth = x.shape[1]
    half = depth // 2 if depth % (2 * LANES) == 0 else depth
    for at in range(0, count, 2 * BLOCK):
        end = min(at + 2 * BLOCK, count)
        total = None
        for k in range(0, depth, half):
            piece = x[:, k : k + half]
            if turned:
                term = jnp.dot(
                    piece, table_ref[k : k + half, at:end], preferred_element_type=jnp.float32
                )
            else:
                term = lax.dot_general(
                    piece, table_ref[at:end, k : k + half], NT, preferred_element_type=jnp.float32
                )
            total = term if total is None else total + term
        put_folded(out_ref, rows, start + at, total)


def vocab_head(own, other, hidden, gain, turned, table, low_row, high_row, width):
    rows, depth = hidden.shape
    fold = fold_of(rows, width)
    count = len(turned)
    pieces = 4
    step = round_up(-(-(high_row - low_row) // pieces), ROW_TILE)

    def kernel(own_ref, other_ref, x_ref, gain_ref, *refs):
        table_ref = refs[count]
        new_ref, scaled_ref, square_ref, out_ref, held, sems, gate = refs[count + 1 :]
        copies = row_copies(table_ref, held, sems, low_row, high_row, step)
        for copy in copies:
            copy.start()
        fence(gate)
        states = x_ref[...].astype(jnp.float32)
        updated = states + get_folded((own_ref, other_ref), rows, 0, depth)
        new_ref[...] = updated.astype(jnp.bfloat16)
        scaled = (updated * gain_ref[...].reshape(1, depth)).astype(jnp.bfloat16)
        scaled_ref[...] = scaled
        square_ref[...] = jnp.broadcast_to(
            jnp.sum(updated * updated, axis=1, keepdims=True), (rows, LANES)
        )
        start = 0
        for turned_ref in refs[:count]:
            put_terms(out_ref, rows, start, scaled, turned_ref, True)
            start += turned_ref.shape[1]
        for copy in copies:
            copy.wait()

    return pl.pallas_call(
        kernel,
        out_shape=(
            jax.ShapeDtypeStruct((rows, depth), jnp.bfloat16),
            jax.ShapeDtypeStruct((rows, depth), jnp.bfloat16),
            jax.ShapeDtypeStruct((rows, LANES), jnp.float32),
            jax.ShapeDtypeStruct((rows * fold, width // fold), jnp.float32),
            pltpu.VMEM((high_row - low_row, depth), table.dtype),
        ),
        in_specs=[VMEM] * (4 + count) + [ANY],
        out_specs=(VMEM,) * 5,
        scratch_shapes=[pltpu.SemaphoreType.DMA((pieces,)), pltpu.SemaphoreType.REGULAR],
        compiler_params=params(3),
        cost_estimate=cost(4),
        name="vocab_head",
    )(own, other, hidden, gain, *[resident(part) for part in turned], stored(table))


def vocab_tail(scaled, square, held_part, table, low_row, high_row, width):
    rows, depth = scaled.shape
    fold = fold_of(rows, width)
    count = high_row - low_row
    used = held_part.shape[0] + count
    step = round_up(-(-count // 2), 2 * BLOCK)
    pieces = -(-count // step)

    def kernel(x_ref, square_ref, held_ref, table_ref, out_ref, late, sems, gate):
        copies = row_copies(table_ref, late, sems, low_row, high_row, step)
        for copy in copies:
            copy.start()
        fence(gate)
        x = x_ref[...]
        put_terms(out_ref, rows, 0, x, held_ref, False)
        start = held_part.shape[0]
        for i, copy in enumerate(copies):
            copy.wait()
            a, b = i * step, min((i + 1) * step, count)
            put_terms(out_ref, rows, start + a, x, late.at[a:b], False)
        put_folded(
            out_ref, rows, used,
            jnp.broadcast_to(square_ref[:, 0:1], (rows, width - used)),
        )

    return pl.pallas_call(
        kernel,
        out_shape=jax.ShapeDtypeStruct((rows * fold, width // fold), jnp.float32),
        in_specs=[VMEM, VMEM, VMEM, ANY],
        out_specs=VMEM,
        scratch_shapes=[
            pltpu.VMEM((count, depth), table.dtype),
            pltpu.SemaphoreType.DMA((pieces,)),
            pltpu.SemaphoreType.REGULAR,
        ],
        compiler_params=params(3 + count * round_up(depth, LANES) * 2 / MIB),
        cost_estimate=cost(6),
        name="vocab_tail",
    )(scaled, square, resident(held_part), stored(table))


def vocab_logits(parts, draft_ids, bounds, rows, features):
    columns = bounds[-1][1]
    count = len(bounds)
    flat = [array for pair in parts for array in pair]

    def kernel(id_ref, *refs):
        pairs = [refs[2 * i : 2 * i + 2] for i in range(count)]
        logit_ref, stat_ref = refs[2 * count :]
        full = pairs[-1][0].shape[0] * pairs[-1][0].shape[1] // rows
        square = get_folded(pairs[-1], rows, full - LANES, LANES)
        inv = lax.rsqrt(square[:, 0:1] / features + EPSILON)
        row = lax.broadcasted_iota(jnp.int32, (rows, 1), 0)
        wanted = jnp.zeros((rows, 1), jnp.int32)
        for r in range(rows):
            wanted = jnp.where(row == r, id_ref[r], wanted)
        wanted = wanted - lax.axis_index("heads") * columns
        top = jnp.full((rows, 1), NEGATIVE, jnp.float32)
        picked = jnp.zeros((rows, 1), jnp.float32)
        for pair, (first, last) in zip(pairs, bounds):
            logits = get_folded(pair, rows, 0, last - first) * inv
            logit_ref[:, first:last] = logits
            top = jnp.maximum(top, jnp.max(logits, axis=1, keepdims=True))
            column = first + lax.broadcasted_iota(jnp.int32, logits.shape, 1)
            picked = picked + jnp.sum(
                jnp.where(column == wanted, logits, 0.0), axis=1, keepdims=True
            )
        total = jnp.zeros((rows, 1), jnp.float32)
        for first, last in bounds:
            total = total + jnp.sum(
                jnp.exp(logit_ref[:, first:last] - top), axis=1, keepdims=True
            )
        lane = lax.broadcasted_iota(jnp.int32, (rows, LANES), 1)
        stat_ref[...] = jnp.where(
            lane == 0, top, jnp.where(lane == 1, total, jnp.where(lane == 2, picked, 0.0))
        )

    return pl.pallas_call(
        kernel,
        out_shape=(
            pltpu.VMEM((rows, columns), jnp.float32),
            jax.ShapeDtypeStruct((rows, LANES), jnp.float32),
        ),
        in_specs=[SMEM] + [VMEM] * len(flat),
        out_specs=(VMEM, VMEM),
        compiler_params=params(4),
        cost_estimate=cost(2),
        name="vocab_logits",
    )(draft_ids, *flat)


def vocab_finish(logits, stats):
    rows, columns = logits.shape
    count = len(stats)

    def kernel(logit_ref, *refs):
        stat_refs, out_ref, draft_ref = refs[:count], refs[count], refs[count + 1]
        state = [(ref[:, 0:1], ref[:, 1:2], ref[:, 2:3]) for ref in stat_refs]
        while len(state) > 1:
            joined = []
            for (top_a, sum_a, pick_a), (top_b, sum_b, pick_b) in zip(state[0::2], state[1::2]):
                top = jnp.maximum(top_a, top_b)
                joined.append(
                    (
                        top,
                        sum_a * jnp.exp(top_a - top) + sum_b * jnp.exp(top_b - top),
                        pick_a + pick_b,
                    )
                )
            state = joined
        top, total, picked = state[0]
        log_total = top + jnp.log(total)
        out_ref[...] = logit_ref[...] - log_total
        draft = picked - log_total
        row = lax.broadcasted_iota(jnp.int32, (rows, LANES), 0)
        lane = lax.broadcasted_iota(jnp.int32, (rows, LANES), 1)
        line = jnp.sum(jnp.where(row == lane, draft, 0.0), axis=0, keepdims=True)
        draft_ref[...] = line[:, 0:rows]

    return pl.pallas_call(
        kernel,
        out_shape=(
            jax.ShapeDtypeStruct((rows, columns), jnp.float32),
            jax.ShapeDtypeStruct((1, rows), jnp.float32),
        ),
        in_specs=[VMEM] * (1 + count),
        out_specs=(VMEM, VMEM),
        compiler_params=params(4),
        cost_estimate=cost(1),
        name="vocab_finish",
    )(resident(logits), *stats)


def pair_sum(array, axis):
    if lax.axis_size(axis) == 2:
        return array, swap(array, axis, 1)
    return lax.psum(array, axis), jnp.zeros_like(array)


def pair_softmax(array, axis, requests, q_width):
    if lax.axis_size(axis) == 2:
        return array, swap(array, axis, 1)
    fold = array.shape[0] // requests
    width = array.shape[1]
    flat = jnp.concatenate(
        [array[i * requests : (i + 1) * requests] for i in range(fold)], axis=1
    )
    every = lax.all_gather(flat, axis)
    tops = every[:, :, q_width : q_width + LANES]
    totals = every[:, :, q_width + LANES :]
    top = jnp.max(tops, axis=0)
    scale = jnp.exp(tops - top)
    heads = q_width // HEAD_DIM
    total = jnp.sum(totals * scale, axis=0)
    mixed = every[:, :, :q_width].reshape(every.shape[0], requests, heads, HEAD_DIM)
    mixed = jnp.sum(mixed * scale[:, :, :heads, None], axis=0).reshape(requests, q_width)
    flat = jnp.concatenate([mixed, top, total], axis=1)
    empty = jnp.concatenate(
        [jnp.zeros_like(mixed), jnp.full_like(top, NEGATIVE), jnp.zeros_like(total)], axis=1
    )

    def folded(value):
        return jnp.concatenate(
            [value[:, i * width : (i + 1) * width] for i in range(fold)], axis=0
        )

    return folded(flat), folded(empty)


def body(
    hidden_in,
    lengths,
    draft_ids,
    input_gain,
    w_query,
    w_latent,
    latent_cache,
    key_up,
    value_up,
    w_out,
    final_gain,
    w_vocab,
):
    rows, depth = hidden_in.shape
    features = depth * lax.axis_size("seq")
    columns = w_vocab.shape[1]
    table = w_vocab.T
    q_width = w_query.shape[1]

    def mark(share):
        return int(columns * share) // BLOCK * BLOCK

    marks = [0, mark(0.16), mark(0.32), mark(0.64), mark(0.832), columns]

    sums = project(
        hidden_in,
        input_gain,
        w_query,
        w_latent.reshape(depth, w_latent.shape[1] * w_latent.shape[2]),
    )
    own, other = pair_sum(sums, "seq")
    cache, keys, values = fetch_attention(
        latent_cache[:, 0], key_up[0], value_up[0], sums, 3
    )
    packed, local, out_table = attend(
        own, other, lengths, cache, keys, values, features, w_out
    )
    own, other = pair_softmax(packed, "seq", rows, q_width)
    turned = [fetch_turned(table, packed, marks[0], marks[1], 3)]
    part = merge_out(own, other, local, out_table, rows)

    heads = lax.axis_size("heads")
    first = part
    if is_power(heads) and heads > 1:
        mask = 1
        while True:
            received = swap(part, "heads", mask)
            mask *= 2
            if mask >= heads:
                break
            part = part + received
    else:
        part, received = lax.psum(part, "heads"), jnp.zeros_like(part)
    turned.append(fetch_turned(table, first, marks[1], marks[2], 3))
    turned.append(fetch_turned(table, part, marks[2], marks[3], 6))

    bounds = [(0, marks[3]), (marks[3], columns)]
    tail_width = round_up(columns - marks[3] + LANES, 2 * LANES)
    new_hidden, scaled, square, piece, late_part = vocab_head(
        part, received, hidden_in, final_gain, turned, table, marks[3], marks[4], marks[3]
    )
    parts = [pair_sum(piece, "seq")]
    piece = vocab_tail(scaled, square, late_part, table, marks[4], columns, tail_width)
    parts.append(pair_sum(piece, "seq"))
    logits, stats = vocab_logits(parts, draft_ids, bounds, rows, features)
    if is_power(heads):
        every = [stats] + [swap(stats, "heads", m) for m in range(1, heads)]
    else:
        gathered = lax.all_gather(stats, "heads")
        every = [gathered[i] for i in range(heads)]
        while not is_power(len(every)):
            every.append(jnp.concatenate([jnp.full_like(stats[:, :1], NEGATIVE), jnp.zeros_like(stats[:, 1:])], axis=1))
    log_probs, draft = vocab_finish(logits, every)
    return (new_hidden, log_probs, draft.reshape(rows))


def solution(mesh):
    return jax.shard_map(
        body,
        mesh=mesh,
        in_specs=(
            P("batch", "seq"),
            P("batch"),
            P("batch"),
            P("seq"),
            P("seq", "heads"),
            P("seq", "heads", None),
            P("batch", "heads", "seq", None),
            P("heads", None, None),
            P("heads", None, None),
            P("heads", "seq"),
            P("seq"),
            P("seq", "heads"),
        ),
        out_specs=(P("batch", "seq"), P("batch", "heads"), P("batch")),
        check_vma=False,
    )
```

```python
import math

import jax
import jax.numpy as jnp
from jax import lax
from jax.experimental import pallas as pl
from jax.experimental.pallas import tpu as pltpu
from jax.sharding import PartitionSpec as P


HEAD_DIM = 128
LANES = 128
ROW_TILE = 16
BLOCK = 256
RING = 6
EPSILON = 1e-05
NEGATIVE = -1e30
MIB = 1 << 20
ANY = pl.BlockSpec(memory_space=pl.ANY)
VMEM = pl.BlockSpec(memory_space=pltpu.VMEM)
SMEM = pl.BlockSpec(memory_space=pltpu.SMEM)
NT = (((1,), (1,)), ((), ()))


def resident(array):
    return pltpu.with_memory_space_constraint(array, pltpu.VMEM)


def stored(array):
    return pltpu.with_memory_space_constraint(array, pltpu.HBM)


def cost(micros):
    return pl.CostEstimate(flops=int(micros * 5e6), bytes_accessed=0, transcendentals=0)


def params(mib):
    return pltpu.CompilerParams(vmem_limit_bytes=int(mib * MIB))


def round_up(value, step):
    return -(-value // step) * step


def fold_of(rows, width):
    fold = 8 // math.gcd(rows, 8)
    return fold if width % (fold * LANES) == 0 else 1


def put_folded(ref, rows, start, value):
    width = ref.shape[1]
    done = 0
    while done < value.shape[1]:
        piece, at = divmod(start + done, width)
        size = min(value.shape[1] - done, width - at)
        ref[piece * rows : (piece + 1) * rows, at : at + size] = value[:, done : done + size]
        done += size


def get_folded(refs, rows, start, size):
    width = refs[0].shape[1]
    pieces = []
    done = 0
    while done < size:
        piece, at = divmod(start + done, width)
        span = min(size - done, width - at)
        block = None
        for ref in refs:
            term = ref[piece * rows : (piece + 1) * rows, at : at + span]
            block = term if block is None else block + term
        pieces.append(block)
        done += span
    return pieces[0] if len(pieces) == 1 else jnp.concatenate(pieces, axis=1)


def swap(array, axis, mask):
    size = lax.axis_size(axis)
    return lax.ppermute(array, axis, [(i, i ^ mask) for i in range(size)])


def fence(sem):
    pl.semaphore_signal(sem, 1)
    pl.semaphore_wait(sem, 1)


def is_power(size):
    return size & (size - 1) == 0


def project(hidden, gain, w_query, w_latent):
    rows, depth = hidden.shape
    q_width, l_width = w_query.shape[1], w_latent.shape[1]
    width = q_width + l_width + LANES
    fold = fold_of(rows, width)
    chunks = 5 if depth % (5 * LANES) == 0 else 1
    step = depth // chunks

    def kernel(x_hbm, gain_hbm, wq_ref, wl_ref, out_ref, x_ref, gain_ref, q_buf, l_buf, sems, ends, gate):
        small = [
            pltpu.make_async_copy(x_hbm, x_ref, ends.at[0]),
            pltpu.make_async_copy(gain_hbm, gain_ref, ends.at[1]),
        ]
        for copy in small:
            copy.start()
        fence(gate)
        copies = []
        for c in range(chunks):
            at = pl.ds(c * step, step)
            copies.append(
                (
                    pltpu.make_async_copy(wq_ref.at[at], q_buf.at[at], sems.at[0, c]),
                    pltpu.make_async_copy(wl_ref.at[at], l_buf.at[at], sems.at[1, c]),
                )
            )
        for pair in copies:
            for copy in pair:
                copy.start()
        for copy in small:
            copy.wait()
        states = x_ref[...].astype(jnp.float32)
        gained = (states * gain_ref[...].reshape(1, depth)).astype(jnp.bfloat16)
        square = jnp.sum(states * states, axis=1, keepdims=True)
        acc_q = acc_l = None
        for c in range(chunks):
            for copy in copies[c]:
                copy.wait()
            x = gained[:, c * step : (c + 1) * step]
            part_q = jnp.dot(
                x, q_buf[c * step : (c + 1) * step, :], preferred_element_type=jnp.float32
            )
            part_l = jnp.dot(
                x, l_buf[c * step : (c + 1) * step, :], preferred_element_type=jnp.float32
            )
            acc_q = part_q if c == 0 else acc_q + part_q
            acc_l = part_l if c == 0 else acc_l + part_l
        put_folded(out_ref, rows, 0, acc_q)
        put_folded(out_ref, rows, q_width, acc_l)
        put_folded(out_ref, rows, q_width + l_width, jnp.broadcast_to(square, (rows, LANES)))

    return pl.pallas_call(
        kernel,
        out_shape=jax.ShapeDtypeStruct((rows * fold, width // fold), jnp.float32),
        in_specs=[ANY] * 4,
        out_specs=VMEM,
        scratch_shapes=[
            pltpu.VMEM(hidden.shape, hidden.dtype),
            pltpu.VMEM(gain.shape, gain.dtype),
            pltpu.VMEM(w_query.shape, w_query.dtype),
            pltpu.VMEM(w_latent.shape, w_latent.dtype),
            pltpu.SemaphoreType.DMA((2, chunks)),
            pltpu.SemaphoreType.DMA((2,)),
            pltpu.SemaphoreType.REGULAR,
        ],
        compiler_params=params(14),
        cost_estimate=cost(5),
        name="project",
    )(stored(hidden), stored(gain), stored(w_query), stored(w_latent))


def row_copies(table_ref, out_ref, sems, low, high, step):
    bounds = [(at, min(at + step, high)) for at in range(low, high, step)]
    return [
        pltpu.make_async_copy(
            table_ref.at[pl.ds(a, b - a)], out_ref.at[pl.ds(a - low, b - a)], sems.at[i]
        )
        for i, (a, b) in enumerate(bounds)
    ]


def turn_copies(table_ref, held_ref, sems, low, high):
    slots = held_ref.shape[0]
    copies = []
    for i, at in enumerate(range(low, high, BLOCK)):
        size = min(BLOCK, high - at)
        copies.append(
            pltpu.make_async_copy(
                table_ref.at[pl.ds(at, size)],
                held_ref.at[i % slots, pl.ds(0, size)],
                sems.at[i % slots],
            )
        )
    return copies


def turn_rows(copies, held_ref, out_ref):
    slots, _, depth = held_ref.shape
    count = out_ref.shape[1]
    for i, copy in enumerate(copies):
        copy.wait()
        a, b = i * BLOCK, min((i + 1) * BLOCK, count)
        for k in range(0, depth, BLOCK):
            end = min(k + BLOCK, depth)
            out_ref[k:end, a:b] = held_ref[i % slots, 0 : b - a, k:end].T
        if i + slots < len(copies):
            copies[i + slots].start()


def turn_slots(count):
    return min(RING, -(-count // BLOCK))


def turn_scratch(table, count):
    return [
        pltpu.VMEM((turn_slots(count), BLOCK, table.shape[1]), table.dtype),
        pltpu.SemaphoreType.DMA((turn_slots(count),)),
    ]


def turn_params(table, count):
    size = turn_slots(count) * BLOCK * round_up(table.shape[1], LANES) * 2
    return params(1 + size / MIB)


def fetch_turned(table, after, low, high, micros):
    def kernel(table_ref, after_ref, out_ref, held, sems):
        copies = turn_copies(table_ref, held, sems, low, high)
        for copy in copies[: held.shape[0]]:
            copy.start()
        turn_rows(copies, held, out_ref)

    return pl.pallas_call(
        kernel,
        out_shape=pltpu.VMEM((table.shape[1], high - low), table.dtype),
        in_specs=[ANY, ANY],
        out_specs=VMEM,
        scratch_shapes=turn_scratch(table, high - low),
        compiler_params=turn_params(table, high - low),
        cost_estimate=cost(micros),
        name="fetch_turned",
    )(stored(table), after)


def fetch_attention(cache, key_up, value_up, table, after, low, high, micros):
    rank, width = value_up.shape
    full = round_up(rank, LANES)

    def kernel(
        cache_ref, key_ref, value_ref, table_ref, after_ref,
        cache_out, key_out, value_out, turned_out, sems, held, row_sems,
    ):
        copies = [
            pltpu.make_async_copy(key_ref, key_out, sems.at[0]),
            pltpu.make_async_copy(value_ref, value_out.at[pl.ds(full - rank, rank)], sems.at[1]),
            pltpu.make_async_copy(cache_ref, cache_out, sems.at[2]),
        ]
        rows = turn_copies(table_ref, held, row_sems, low, high)
        for copy in rows[: held.shape[0]] + copies:
            copy.start()
        value_out[0 : full - rank, :] = jnp.zeros((full - rank, width), value_up.dtype)
        turn_rows(rows, held, turned_out)
        for copy in copies:
            copy.wait()

    return pl.pallas_call(
        kernel,
        out_shape=(
            pltpu.VMEM(cache.shape, cache.dtype),
            pltpu.VMEM(key_up.shape, key_up.dtype),
            pltpu.VMEM((full, width), value_up.dtype),
            pltpu.VMEM((table.shape[1], high - low), table.dtype),
        ),
        in_specs=[ANY] * 5,
        out_specs=(VMEM,) * 4,
        scratch_shapes=[pltpu.SemaphoreType.DMA((3,))] + turn_scratch(table, high - low),
        compiler_params=turn_params(table, high - low),
        cost_estimate=cost(micros),
        name="fetch_attention",
    )(stored(cache), stored(key_up), stored(value_up), stored(table), after)


def attend(own, other, lengths, cache, key_up, value_pad, features, w_out):
    requests, span, width = cache.shape
    rank = width // 2
    full = value_pad.shape[0]
    low = width - full
    heads = key_up.shape[1] // HEAD_DIM
    slot = round_up(heads, ROW_TILE)
    scaling = 1.0 / math.sqrt(HEAD_DIM)
    q_width = heads * HEAD_DIM
    send_width = q_width + 2 * LANES
    fold = fold_of(requests, send_width)

    def kernel(
        own_ref, other_ref, length_ref, cache_ref, key_ref, value_ref, w_ref,
        send_ref, local_ref, w_held, sems, gate, score_own, top_buf, total_buf, latent_buf, stack,
        score_buf, weight_buf, *tiles,
    ):
        absorbed, mixed = tiles[: full // LANES], tiles[full // LANES :]
        copies = row_copies(w_ref, w_held, sems, 0, w_out.shape[0], w_out.shape[0] // 2)
        for copy in copies:
            copy.start()
        fence(gate)
        refs = (own_ref, other_ref)
        square = get_folded(refs, requests, q_width + width, LANES)
        inv = lax.rsqrt(square[:, 0:1] / features + EPSILON)
        query = (inv * get_folded(refs, requests, 0, q_width)).astype(jnp.bfloat16)
        latent = (inv * get_folded(refs, requests, q_width, width)).astype(jnp.bfloat16)
        latent_buf[...] = latent.astype(jnp.float32)
        for tile in absorbed:
            tile[...] = jnp.zeros(tile.shape, jnp.float32)
        for j in range(heads):
            at = slice(j * HEAD_DIM, (j + 1) * HEAD_DIM)
            row = lax.dot_general(
                query[:, at], key_ref[:, at], NT, preferred_element_type=jnp.float32
            )
            row = row.astype(jnp.bfloat16).astype(jnp.float32)
            for i, tile in enumerate(absorbed):
                piece = row[:, i * LANES : min((i + 1) * LANES, rank)]
                if piece.shape[1] < LANES:
                    edge = jnp.zeros((requests, LANES - piece.shape[1]), jnp.float32)
                    piece = jnp.concatenate([piece, edge], axis=1)
                tile[pl.ds(j, requests, stride=slot), :] = piece
        first = lax.axis_index("seq") * span
        positions = first + lax.broadcasted_iota(jnp.int32, (slot, span), 1)
        spans = [slice(b * slot, (b + 1) * slot) for b in range(requests)]
        for b, at in enumerate(spans):
            rows = jnp.concatenate([tile[at, :] for tile in absorbed], axis=1)
            score_buf[at, :] = lax.dot_general(
                rows.astype(jnp.bfloat16),
                cache_ref[b, :, 0:full],
                NT,
                preferred_element_type=jnp.float32,
            )
            score_own[at, :] = jnp.broadcast_to(
                jnp.sum(rows * latent_buf[b : b + 1, 0:full], axis=1, keepdims=True) * scaling,
                (slot, LANES),
            )
        for b, at in enumerate(spans):
            live = positions < length_ref[b]
            scores = jnp.where(live, score_buf[at, :] * scaling, NEGATIVE)
            top = jnp.max(scores, axis=1, keepdims=True)
            weights = jnp.where(live, jnp.exp(scores - top), 0.0)
            top_buf[at, :] = jnp.broadcast_to(top, (slot, LANES))
            total_buf[at, :] = jnp.broadcast_to(
                jnp.sum(weights, axis=1, keepdims=True), (slot, LANES)
            )
            weight_buf[at, :] = weights.astype(jnp.bfloat16)
        for b, at in enumerate(spans):
            value = jnp.dot(
                weight_buf[at, :], cache_ref[b, :, low:width], preferred_element_type=jnp.float32
            )
            for i, tile in enumerate(mixed):
                tile[at, :] = value[:, i * LANES : (i + 1) * LANES]
        lane = lax.broadcasted_iota(jnp.int32, (requests, LANES), 1)
        tops = jnp.full((requests, LANES), NEGATIVE, jnp.float32)
        owns = jnp.full((requests, LANES), NEGATIVE, jnp.float32)
        totals = jnp.zeros((requests, LANES), jnp.float32)
        second = ROW_TILE * -(-requests // ROW_TILE)
        stack[2 * second : 2 * second + requests, :] = latent[:, low:width]
        for j in range(heads):
            pick = pl.ds(j, requests, stride=slot)
            tops = jnp.where(lane == j, top_buf[pick, :], tops)
            totals = jnp.where(lane == j, total_buf[pick, :], totals)
            owns = jnp.where(lane == j, score_own[pick, :], owns)
            value = jnp.concatenate([tile[pick, :] for tile in mixed], axis=1)
            high = value.astype(jnp.bfloat16)
            stack[0:requests, :] = high
            stack[second : second + requests, :] = (value - high.astype(jnp.float32)).astype(
                jnp.bfloat16
            )
            at = slice(j * HEAD_DIM, (j + 1) * HEAD_DIM)
            lifted = jnp.dot(stack[...], value_ref[:, at], preferred_element_type=jnp.float32)
            put_folded(
                send_ref, requests, j * HEAD_DIM,
                lifted[0:requests] + lifted[second : second + requests],
            )
            local_ref[:, at] = lifted[2 * second : 2 * second + requests]
        put_folded(send_ref, requests, q_width, tops)
        put_folded(send_ref, requests, q_width + LANES, totals)
        local_ref[:, q_width : q_width + LANES] = owns
        for copy in copies:
            copy.wait()

    tall = requests * slot
    return pl.pallas_call(
        kernel,
        out_shape=(
            jax.ShapeDtypeStruct((requests * fold, send_width // fold), jnp.float32),
            jax.ShapeDtypeStruct((requests, q_width + LANES), jnp.float32),
            pltpu.VMEM(w_out.shape, w_out.dtype),
        ),
        in_specs=[VMEM, VMEM, SMEM, VMEM, VMEM, VMEM, ANY],
        out_specs=(VMEM,) * 3,
        scratch_shapes=[
            pltpu.SemaphoreType.DMA((2,)),
            pltpu.SemaphoreType.REGULAR,
            pltpu.VMEM((tall, LANES), jnp.float32),
            pltpu.VMEM((tall, LANES), jnp.float32),
            pltpu.VMEM((tall, LANES), jnp.float32),
            pltpu.VMEM((requests, width), jnp.float32),
            pltpu.VMEM((3 * round_up(requests, ROW_TILE), full), jnp.bfloat16),
            pltpu.VMEM((tall, span), jnp.float32),
            pltpu.VMEM((tall, span), jnp.bfloat16),
        ]
        + [pltpu.VMEM((tall, LANES), jnp.float32)] * (2 * full // LANES),
        compiler_params=params(5),
        cost_estimate=cost(5),
        name="attend",
    )(
        own, other, lengths, resident(cache), resident(key_up), resident(value_pad),
        stored(w_out),
    )


def merge_out(own, other, local, w_out, requests):
    q_width = local.shape[1] - LANES
    heads = q_width // HEAD_DIM
    width = w_out.shape[1]
    fold = fold_of(requests, width)
    step = 512 if width % 512 == 0 else width

    def kernel(own_ref, other_ref, local_ref, w_ref, out_ref, head_buf):
        top_a = get_folded((own_ref,), requests, q_width, LANES)
        top_b = get_folded((other_ref,), requests, q_width, LANES)
        total_a = get_folded((own_ref,), requests, q_width + LANES, LANES)
        total_b = get_folded((other_ref,), requests, q_width + LANES, LANES)
        own_score = local_ref[:, q_width : q_width + LANES]
        highest = jnp.maximum(jnp.maximum(top_a, top_b), own_score)
        scale_a = jnp.exp(top_a - highest)
        scale_b = jnp.exp(top_b - highest)
        own_weight = jnp.exp(own_score - highest)
        below = total_a * scale_a + total_b * scale_b + own_weight
        scale_a = scale_a / below
        scale_b = scale_b / below
        own_weight = own_weight / below
        for j in range(heads):
            at = slice(j * HEAD_DIM, (j + 1) * HEAD_DIM)
            value = (
                get_folded((own_ref,), requests, j * HEAD_DIM, HEAD_DIM) * scale_a[:, j : j + 1]
                + get_folded((other_ref,), requests, j * HEAD_DIM, HEAD_DIM)
                * scale_b[:, j : j + 1]
                + local_ref[:, at] * own_weight[:, j : j + 1]
            )
            head_buf[:, at] = value.astype(jnp.bfloat16)
        head_out = head_buf[...]
        for at in range(0, width, step):
            put_folded(
                out_ref, requests, at,
                jnp.dot(head_out, w_ref[:, at : at + step], preferred_element_type=jnp.float32),
            )

    return pl.pallas_call(
        kernel,
        out_shape=jax.ShapeDtypeStruct((requests * fold, width // fold), jnp.float32),
        in_specs=[VMEM] * 4,
        out_specs=VMEM,
        scratch_shapes=[pltpu.VMEM((requests, q_width), jnp.bfloat16)],
        compiler_params=params(3),
        cost_estimate=cost(2),
        name="merge_out",
    )(own, other, local, resident(w_out))


def put_terms(out_ref, rows, x, parts, low, high):
    depth = x.shape[1]
    half = depth // 2 if depth % (2 * LANES) == 0 else depth
    base = 0
    for ref, turned in parts:
        count = ref.shape[1] if turned else ref.shape[0]
        first, last = max(low, base), min(high, base + count)
        for at in range(first, last, 2 * BLOCK):
            a, b = at - base, min(at + 2 * BLOCK, last) - base
            total = None
            for k in range(0, depth, half):
                piece = x[:, k : k + half]
                if turned:
                    term = jnp.dot(
                        piece, ref[k : k + half, a:b], preferred_element_type=jnp.float32
                    )
                else:
                    term = lax.dot_general(
                        piece, ref[a:b, k : k + half], NT, preferred_element_type=jnp.float32
                    )
                total = term if total is None else total + term
            put_folded(out_ref, rows, at - low, total)
        base += count


def vocab_head(own, other, hidden, gain, turned, split, table, low_row, high_row, width):
    rows, depth = hidden.shape
    fold = fold_of(rows, width)
    count = len(turned)
    pieces = 2
    step = round_up(-(-(high_row - low_row) // pieces), ROW_TILE)

    def kernel(own_ref, other_ref, x_ref, gain_ref, *refs):
        table_ref = refs[count]
        new_ref, scaled_ref, out_ref, held, sems, gate = refs[count + 1 :]
        copies = row_copies(table_ref, held, sems, low_row, high_row, step)
        for copy in copies:
            copy.start()
        fence(gate)
        states = x_ref[...].astype(jnp.float32)
        updated = states + get_folded((own_ref, other_ref), rows, 0, depth)
        new_ref[...] = updated.astype(jnp.bfloat16)
        scaled = (updated * gain_ref[...].reshape(1, depth)).astype(jnp.bfloat16)
        scaled_ref[...] = scaled
        square = jnp.sum(updated * updated, axis=1, keepdims=True)
        put_folded(out_ref, rows, split, jnp.broadcast_to(square, (rows, width - split)))
        put_terms(out_ref, rows, scaled, [(ref, True) for ref in refs[:count]], 0, split)
        for copy in copies:
            copy.wait()

    return pl.pallas_call(
        kernel,
        out_shape=(
            jax.ShapeDtypeStruct((rows, depth), jnp.bfloat16),
            jax.ShapeDtypeStruct((rows, depth), jnp.bfloat16),
            jax.ShapeDtypeStruct((rows * fold, width // fold), jnp.float32),
            pltpu.VMEM((high_row - low_row, depth), table.dtype),
        ),
        in_specs=[VMEM] * (4 + count) + [ANY],
        out_specs=(VMEM,) * 4,
        scratch_shapes=[pltpu.SemaphoreType.DMA((pieces,)), pltpu.SemaphoreType.REGULAR],
        compiler_params=params(3),
        cost_estimate=cost(4),
        name="vocab_head",
    )(own, other, hidden, gain, *[resident(part) for part in turned], stored(table))


def vocab_tail(scaled, turned, late_part, split, columns, width):
    rows = scaled.shape[0]
    fold = fold_of(rows, width)
    count = len(turned)

    def kernel(x_ref, *refs):
        late_ref, out_ref = refs[count:]
        used = columns - split
        if used < width:
            put_folded(out_ref, rows, used, jnp.zeros((rows, width - used), jnp.float32))
        parts = [(ref, True) for ref in refs[:count]] + [(late_ref, False)]
        put_terms(out_ref, rows, x_ref[...], parts, split, columns)

    return pl.pallas_call(
        kernel,
        out_shape=jax.ShapeDtypeStruct((rows * fold, width // fold), jnp.float32),
        in_specs=[VMEM] * (2 + count),
        out_specs=VMEM,
        compiler_params=params(3),
        cost_estimate=cost(6),
        name="vocab_tail",
    )(scaled, *[resident(part) for part in turned], resident(late_part))


def vocab_front(own, other, draft_ids, last, columns, features):
    rows = draft_ids.shape[0]
    width = own.shape[0] * own.shape[1] // rows

    def kernel(id_ref, own_ref, other_ref, logit_ref, stat_ref):
        pair = (own_ref, other_ref)
        square = get_folded(pair, rows, width - LANES, LANES)
        inv = lax.rsqrt(square[:, 0:1] / features + EPSILON)
        row = lax.broadcasted_iota(jnp.int32, (rows, 1), 0)
        wanted = jnp.zeros((rows, 1), jnp.int32)
        for r in range(rows):
            wanted = jnp.where(row == r, id_ref[r], wanted)
        wanted = wanted - lax.axis_index("heads") * columns
        logits = get_folded(pair, rows, 0, last) * inv
        logit_ref[...] = logits
        column = lax.broadcasted_iota(jnp.int32, logits.shape, 1)
        picked = jnp.sum(jnp.where(column == wanted, logits, 0.0), axis=1, keepdims=True)
        top = jnp.max(logits, axis=1, keepdims=True)
        total = jnp.sum(jnp.exp(logits - top), axis=1, keepdims=True)
        lane = lax.broadcasted_iota(jnp.int32, (rows, LANES), 1)
        stats = jnp.where(lane == 1, total, jnp.where(lane == 2, picked, inv))
        stat_ref[0:rows, :] = jnp.where(lane == 0, top, stats)
        stat_ref[rows : 2 * rows, :] = jnp.broadcast_to(wanted, (rows, LANES)).astype(jnp.float32)

    return pl.pallas_call(
        kernel,
        out_shape=(
            pltpu.VMEM((rows, last), jnp.float32),
            jax.ShapeDtypeStruct((2 * rows, LANES), jnp.float32),
        ),
        in_specs=[SMEM, VMEM, VMEM],
        out_specs=(VMEM, VMEM),
        compiler_params=params(4),
        cost_estimate=cost(1),
        name="vocab_front",
    )(draft_ids, own, other)


def vocab_back(own, other, front_stats, first, count):
    rows = front_stats.shape[0] // 2

    def kernel(front_ref, own_ref, other_ref, logit_ref, stat_ref):
        top_front, total_front = front_ref[0:rows, 0:1], front_ref[0:rows, 1:2]
        picked_front, inv = front_ref[0:rows, 2:3], front_ref[0:rows, 3:4]
        wanted = front_ref[rows : 2 * rows, 0:1].astype(jnp.int32)
        logits = get_folded((own_ref, other_ref), rows, 0, count) * inv
        logit_ref[...] = logits
        column = first + lax.broadcasted_iota(jnp.int32, logits.shape, 1)
        picked = picked_front + jnp.sum(
            jnp.where(column == wanted, logits, 0.0), axis=1, keepdims=True
        )
        top = jnp.maximum(top_front, jnp.max(logits, axis=1, keepdims=True))
        total = total_front * jnp.exp(top_front - top) + jnp.sum(
            jnp.exp(logits - top), axis=1, keepdims=True
        )
        lane = lax.broadcasted_iota(jnp.int32, (rows, LANES), 1)
        stat_ref[...] = jnp.where(
            lane == 0, top, jnp.where(lane == 1, total, jnp.where(lane == 2, picked, 0.0))
        )

    return pl.pallas_call(
        kernel,
        out_shape=(
            pltpu.VMEM((rows, count), jnp.float32),
            jax.ShapeDtypeStruct((rows, LANES), jnp.float32),
        ),
        in_specs=[VMEM] * 3,
        out_specs=(VMEM, VMEM),
        compiler_params=params(4),
        cost_estimate=cost(1),
        name="vocab_back",
    )(front_stats, own, other)


def vocab_finish(front, back, stats):
    rows, split = front.shape
    columns = split + back.shape[1]
    count = len(stats)

    def kernel(front_ref, back_ref, *refs):
        stat_refs, out_ref, draft_ref = refs[:count], refs[count], refs[count + 1]
        state = [(ref[:, 0:1], ref[:, 1:2], ref[:, 2:3]) for ref in stat_refs]
        while len(state) > 1:
            joined = []
            for (top_a, sum_a, pick_a), (top_b, sum_b, pick_b) in zip(state[0::2], state[1::2]):
                top = jnp.maximum(top_a, top_b)
                joined.append(
                    (
                        top,
                        sum_a * jnp.exp(top_a - top) + sum_b * jnp.exp(top_b - top),
                        pick_a + pick_b,
                    )
                )
            state = joined
        top, total, picked = state[0]
        log_total = top + jnp.log(total)
        out_ref[:, 0:split] = front_ref[...] - log_total
        out_ref[:, split:columns] = back_ref[...] - log_total
        draft = picked - log_total
        row = lax.broadcasted_iota(jnp.int32, (rows, LANES), 0)
        lane = lax.broadcasted_iota(jnp.int32, (rows, LANES), 1)
        line = jnp.sum(jnp.where(row == lane, draft, 0.0), axis=0, keepdims=True)
        draft_ref[...] = line[:, 0:rows]

    return pl.pallas_call(
        kernel,
        out_shape=(
            jax.ShapeDtypeStruct((rows, columns), jnp.float32),
            jax.ShapeDtypeStruct((1, rows), jnp.float32),
        ),
        in_specs=[VMEM] * (2 + count),
        out_specs=(VMEM, VMEM),
        compiler_params=params(4),
        cost_estimate=cost(1),
        name="vocab_finish",
    )(resident(front), resident(back), *stats)


def pair_sum(array, axis):
    if lax.axis_size(axis) == 2:
        return array, swap(array, axis, 1)
    return lax.psum(array, axis), jnp.zeros_like(array)


def pair_softmax(array, axis, requests, q_width):
    if lax.axis_size(axis) == 2:
        return array, swap(array, axis, 1)
    fold = array.shape[0] // requests
    width = array.shape[1]
    flat = jnp.concatenate(
        [array[i * requests : (i + 1) * requests] for i in range(fold)], axis=1
    )
    every = lax.all_gather(flat, axis)
    tops = every[:, :, q_width : q_width + LANES]
    totals = every[:, :, q_width + LANES :]
    top = jnp.max(tops, axis=0)
    scale = jnp.exp(tops - top)
    heads = q_width // HEAD_DIM
    total = jnp.sum(totals * scale, axis=0)
    mixed = every[:, :, :q_width].reshape(every.shape[0], requests, heads, HEAD_DIM)
    mixed = jnp.sum(mixed * scale[:, :, :heads, None], axis=0).reshape(requests, q_width)
    flat = jnp.concatenate([mixed, top, total], axis=1)
    empty = jnp.concatenate(
        [jnp.zeros_like(mixed), jnp.full_like(top, NEGATIVE), jnp.zeros_like(total)], axis=1
    )

    def folded(value):
        return jnp.concatenate(
            [value[:, i * width : (i + 1) * width] for i in range(fold)], axis=0
        )

    return folded(flat), folded(empty)


def body(
    hidden_in,
    lengths,
    draft_ids,
    input_gain,
    w_query,
    w_latent,
    latent_cache,
    key_up,
    value_up,
    w_out,
    final_gain,
    w_vocab,
):
    rows, depth = hidden_in.shape
    features = depth * lax.axis_size("seq")
    columns = w_vocab.shape[1]
    table = w_vocab.T
    q_width = w_query.shape[1]

    def mark(share):
        return int(columns * share) // BLOCK * BLOCK

    marks = [0, mark(0.096), mark(0.288), mark(0.512), mark(0.896), columns]
    split = mark(0.448)

    sums = project(
        hidden_in,
        input_gain,
        w_query,
        w_latent.reshape(depth, w_latent.shape[1] * w_latent.shape[2]),
    )
    own, other = pair_sum(sums, "seq")
    cache, keys, values, turned = fetch_attention(
        latent_cache[:, 0], key_up[0], value_up[0], table, sums, marks[0], marks[1], 3
    )
    turned = [turned]
    packed, local, out_table = attend(
        own, other, lengths, cache, keys, values, features, w_out
    )
    own, other = pair_softmax(packed, "seq", rows, q_width)
    turned.append(fetch_turned(table, packed, marks[1], marks[2], 3))
    part = merge_out(own, other, local, out_table, rows)

    heads = lax.axis_size("heads")
    first = part
    if is_power(heads) and heads > 1:
        mask = 1
        while True:
            received = swap(part, "heads", mask)
            mask *= 2
            if mask >= heads:
                break
            part = part + received
    else:
        part, received = lax.psum(part, "heads"), jnp.zeros_like(part)
    turned.append(fetch_turned(table, first, marks[2], marks[3], 3))
    turned.append(fetch_turned(table, part, marks[3], marks[4], 6))

    new_hidden, scaled, piece, late_part = vocab_head(
        part, received, hidden_in, final_gain,
        turned, split,
        table, marks[4], columns, round_up(split + LANES, 2 * LANES),
    )
    own, other = pair_sum(piece, "seq")
    piece = vocab_tail(
        scaled, turned, late_part, split, columns, round_up(columns - split, 2 * LANES)
    )
    front, front_stats = vocab_front(own, other, draft_ids, split, columns, features)
    own, other = pair_sum(piece, "seq")
    back, stats = vocab_back(own, other, front_stats, split, columns - split)
    if is_power(heads):
        every = [stats] + [swap(stats, "heads", m) for m in range(1, heads)]
    else:
        gathered = lax.all_gather(stats, "heads")
        every = [gathered[i] for i in range(heads)]
        while not is_power(len(every)):
            every.append(jnp.concatenate([jnp.full_like(stats[:, :1], NEGATIVE), jnp.zeros_like(stats[:, 1:])], axis=1))
    log_probs, draft = vocab_finish(front, back, every)
    return (new_hidden, log_probs, draft.reshape(rows))


def solution(mesh):
    return jax.shard_map(
        body,
        mesh=mesh,
        in_specs=(
            P("batch", "seq"),
            P("batch"),
            P("batch"),
            P("seq"),
            P("seq", "heads"),
            P("seq", "heads", None),
            P("batch", "heads", "seq", None),
            P("heads", None, None),
            P("heads", None, None),
            P("heads", "seq"),
            P("seq"),
            P("seq", "heads"),
        ),
        out_specs=(P("batch", "seq"), P("batch", "heads"), P("batch")),
        check_vma=False,
    )
```

```python
import math

import jax
import jax.numpy as jnp
from jax import lax
from jax.experimental import pallas as pl
from jax.experimental.pallas import tpu as pltpu
from jax.sharding import PartitionSpec as P


HEAD_DIM = 128
LANES = 128
ROW_TILE = 16
BLOCK = 256
RING = 6
LATE = 2
EPSILON = 1e-05
NEGATIVE = -1e30
MIB = 1 << 20
ANY = pl.BlockSpec(memory_space=pl.ANY)
VMEM = pl.BlockSpec(memory_space=pltpu.VMEM)
SMEM = pl.BlockSpec(memory_space=pltpu.SMEM)
NT = (((1,), (1,)), ((), ()))


def resident(array):
    return pltpu.with_memory_space_constraint(array, pltpu.VMEM)


def stored(array):
    return pltpu.with_memory_space_constraint(array, pltpu.HBM)


def cost(micros):
    return pl.CostEstimate(flops=int(micros * 5e6), bytes_accessed=0, transcendentals=0)


def params(mib):
    return pltpu.CompilerParams(vmem_limit_bytes=int(mib * MIB))


def round_up(value, step):
    return -(-value // step) * step


def fold_of(rows, width):
    fold = 8 // math.gcd(rows, 8)
    return fold if width % (fold * LANES) == 0 else 1


def put_folded(ref, rows, start, value):
    width = ref.shape[1]
    done = 0
    while done < value.shape[1]:
        piece, at = divmod(start + done, width)
        size = min(value.shape[1] - done, width - at)
        ref[piece * rows : (piece + 1) * rows, at : at + size] = value[:, done : done + size]
        done += size


def get_folded(refs, rows, start, size):
    width = refs[0].shape[1]
    pieces = []
    done = 0
    while done < size:
        piece, at = divmod(start + done, width)
        span = min(size - done, width - at)
        block = None
        for ref in refs:
            term = ref[piece * rows : (piece + 1) * rows, at : at + span]
            block = term if block is None else block + term
        pieces.append(block)
        done += span
    return pieces[0] if len(pieces) == 1 else jnp.concatenate(pieces, axis=1)


def swap(array, axis, mask):
    size = lax.axis_size(axis)
    return lax.ppermute(array, axis, [(i, i ^ mask) for i in range(size)])


def fence(sem):
    pl.semaphore_signal(sem, 1)
    pl.semaphore_wait(sem, 1)


def is_power(size):
    return size & (size - 1) == 0


def project(hidden, gain, w_query, w_latent):
    rows, depth = hidden.shape
    q_width, l_width = w_query.shape[1], w_latent.shape[1]
    width = q_width + l_width + LANES
    fold = fold_of(rows, width)
    chunks = 5 if depth % (5 * LANES) == 0 else 1
    spans = [(depth * i // chunks, depth * (i + 1) // chunks) for i in range(chunks)]

    def kernel(x_hbm, gain_hbm, wq_ref, wl_ref, out_ref, x_ref, gain_ref, q_buf, l_buf, sems, ends, gate):
        small = [
            pltpu.make_async_copy(x_hbm, x_ref, ends.at[0]),
            pltpu.make_async_copy(gain_hbm, gain_ref, ends.at[1]),
        ]
        for copy in small:
            copy.start()
        fence(gate)
        copies = []
        for c, (a, b) in enumerate(spans):
            at = pl.ds(a, b - a)
            copies.append(
                (
                    pltpu.make_async_copy(wq_ref.at[at], q_buf.at[at], sems.at[0, c]),
                    pltpu.make_async_copy(wl_ref.at[at], l_buf.at[at], sems.at[1, c]),
                )
            )
        for pair in copies:
            for copy in pair:
                copy.start()
        for copy in small:
            copy.wait()
        states = x_ref[...].astype(jnp.float32)
        gained = (states * gain_ref[...].reshape(1, depth)).astype(jnp.bfloat16)
        square = jnp.sum(states * states, axis=1, keepdims=True)
        acc_q = acc_l = None
        for c, (a, b) in enumerate(spans):
            for copy in copies[c]:
                copy.wait()
            x = gained[:, a:b]
            part_q = jnp.dot(x, q_buf[a:b, :], preferred_element_type=jnp.float32)
            part_l = jnp.dot(x, l_buf[a:b, :], preferred_element_type=jnp.float32)
            acc_q = part_q if c == 0 else acc_q + part_q
            acc_l = part_l if c == 0 else acc_l + part_l
        put_folded(out_ref, rows, 0, acc_q)
        put_folded(out_ref, rows, q_width, acc_l)
        put_folded(out_ref, rows, q_width + l_width, jnp.broadcast_to(square, (rows, LANES)))

    return pl.pallas_call(
        kernel,
        out_shape=jax.ShapeDtypeStruct((rows * fold, width // fold), jnp.float32),
        in_specs=[ANY] * 4,
        out_specs=VMEM,
        scratch_shapes=[
            pltpu.VMEM(hidden.shape, hidden.dtype),
            pltpu.VMEM(gain.shape, gain.dtype),
            pltpu.VMEM(w_query.shape, w_query.dtype),
            pltpu.VMEM(w_latent.shape, w_latent.dtype),
            pltpu.SemaphoreType.DMA((2, chunks)),
            pltpu.SemaphoreType.DMA((2,)),
            pltpu.SemaphoreType.REGULAR,
        ],
        compiler_params=params(14),
        cost_estimate=cost(5),
        name="project",
    )(stored(hidden), stored(gain), stored(w_query), stored(w_latent))


def row_copies(table_ref, out_ref, sems, low, high, step):
    bounds = [(at, min(at + step, high)) for at in range(low, high, step)]
    return [
        pltpu.make_async_copy(
            table_ref.at[pl.ds(a, b - a)], out_ref.at[pl.ds(a - low, b - a)], sems.at[i]
        )
        for i, (a, b) in enumerate(bounds)
    ]


def turn_copies(table_ref, held_ref, sems, low, high):
    slots = held_ref.shape[0]
    copies = []
    for i, at in enumerate(range(low, high, BLOCK)):
        size = min(BLOCK, high - at)
        copies.append(
            pltpu.make_async_copy(
                table_ref.at[pl.ds(at, size)],
                held_ref.at[i % slots, pl.ds(0, size)],
                sems.at[i % slots],
            )
        )
    return copies


def turn_rows(copies, held_ref, out_ref):
    slots, _, depth = held_ref.shape
    count = out_ref.shape[1]
    for i, copy in enumerate(copies):
        copy.wait()
        a, b = i * BLOCK, min((i + 1) * BLOCK, count)
        for k in range(0, depth, BLOCK):
            end = min(k + BLOCK, depth)
            out_ref[k:end, a:b] = held_ref[i % slots, 0 : b - a, k:end].T
        if i + slots < len(copies):
            copies[i + slots].start()


def turn_slots(count):
    return min(RING, -(-count // BLOCK))


def turn_scratch(table, count):
    return [
        pltpu.VMEM((turn_slots(count), BLOCK, table.shape[1]), table.dtype),
        pltpu.SemaphoreType.DMA((turn_slots(count),)),
    ]


def turn_params(table, count):
    size = turn_slots(count) * BLOCK * round_up(table.shape[1], LANES) * 2
    return params(1 + size / MIB)


def fetch_turned(table, after, low, high, micros):
    def kernel(table_ref, after_ref, out_ref, held, sems):
        copies = turn_copies(table_ref, held, sems, low, high)
        for copy in copies[: held.shape[0]]:
            copy.start()
        turn_rows(copies, held, out_ref)

    return pl.pallas_call(
        kernel,
        out_shape=pltpu.VMEM((table.shape[1], high - low), table.dtype),
        in_specs=[ANY, ANY],
        out_specs=VMEM,
        scratch_shapes=turn_scratch(table, high - low),
        compiler_params=turn_params(table, high - low),
        cost_estimate=cost(micros),
        name="fetch_turned",
    )(stored(table), after)


def fetch_attention(cache, key_up, value_up, table, after, low, high, micros):
    rank, width = value_up.shape
    full = round_up(rank, LANES)

    def kernel(
        cache_ref, key_ref, value_ref, table_ref, after_ref,
        cache_out, key_out, value_out, turned_out, sems, held, row_sems,
    ):
        copies = [
            pltpu.make_async_copy(key_ref, key_out, sems.at[0]),
            pltpu.make_async_copy(value_ref, value_out.at[pl.ds(full - rank, rank)], sems.at[1]),
            pltpu.make_async_copy(cache_ref, cache_out, sems.at[2]),
        ]
        rows = turn_copies(table_ref, held, row_sems, low, high)
        for copy in rows[: held.shape[0]] + copies:
            copy.start()
        value_out[0 : full - rank, :] = jnp.zeros((full - rank, width), value_up.dtype)
        turn_rows(rows, held, turned_out)
        for copy in copies:
            copy.wait()

    return pl.pallas_call(
        kernel,
        out_shape=(
            pltpu.VMEM(cache.shape, cache.dtype),
            pltpu.VMEM(key_up.shape, key_up.dtype),
            pltpu.VMEM((full, width), value_up.dtype),
            pltpu.VMEM((table.shape[1], high - low), table.dtype),
        ),
        in_specs=[ANY] * 5,
        out_specs=(VMEM,) * 4,
        scratch_shapes=[pltpu.SemaphoreType.DMA((3,))] + turn_scratch(table, high - low),
        compiler_params=turn_params(table, high - low),
        cost_estimate=cost(micros),
        name="fetch_attention",
    )(stored(cache), stored(key_up), stored(value_up), stored(table), after)


def attend(own, other, lengths, cache, key_up, value_pad, features):
    requests, span, width = cache.shape
    rank = width // 2
    full = value_pad.shape[0]
    low = width - full
    heads = key_up.shape[1] // HEAD_DIM
    slot = round_up(heads, ROW_TILE)
    scaling = 1.0 / math.sqrt(HEAD_DIM)
    q_width = heads * HEAD_DIM
    send_width = q_width + 2 * LANES
    fold = fold_of(requests, send_width)

    def kernel(
        own_ref, other_ref, length_ref, cache_ref, key_ref, value_ref,
        send_ref, local_ref, score_own, top_buf, total_buf, latent_buf, stack,
        score_buf, weight_buf, *tiles,
    ):
        absorbed, mixed = tiles[: full // LANES], tiles[full // LANES :]
        refs = (own_ref, other_ref)
        square = get_folded(refs, requests, q_width + width, LANES)
        inv = lax.rsqrt(square[:, 0:1] / features + EPSILON)
        query = (inv * get_folded(refs, requests, 0, q_width)).astype(jnp.bfloat16)
        latent = (inv * get_folded(refs, requests, q_width, width)).astype(jnp.bfloat16)
        latent_buf[...] = latent.astype(jnp.float32)
        for tile in absorbed:
            tile[...] = jnp.zeros(tile.shape, jnp.float32)
        for j in range(heads):
            at = slice(j * HEAD_DIM, (j + 1) * HEAD_DIM)
            row = lax.dot_general(
                query[:, at], key_ref[:, at], NT, preferred_element_type=jnp.float32
            )
            row = row.astype(jnp.bfloat16).astype(jnp.float32)
            for i, tile in enumerate(absorbed):
                piece = row[:, i * LANES : min((i + 1) * LANES, rank)]
                if piece.shape[1] < LANES:
                    edge = jnp.zeros((requests, LANES - piece.shape[1]), jnp.float32)
                    piece = jnp.concatenate([piece, edge], axis=1)
                tile[pl.ds(j, requests, stride=slot), :] = piece
        first = lax.axis_index("seq") * span
        positions = first + lax.broadcasted_iota(jnp.int32, (slot, span), 1)
        spans = [slice(b * slot, (b + 1) * slot) for b in range(requests)]
        for b, at in enumerate(spans):
            rows = jnp.concatenate([tile[at, :] for tile in absorbed], axis=1)
            score_buf[at, :] = lax.dot_general(
                rows.astype(jnp.bfloat16),
                cache_ref[b, :, 0:full],
                NT,
                preferred_element_type=jnp.float32,
            )
            score_own[at, :] = jnp.broadcast_to(
                jnp.sum(rows * latent_buf[b : b + 1, 0:full], axis=1, keepdims=True) * scaling,
                (slot, LANES),
            )
        lengths_row = length_ref[...].reshape(1, requests)
        for b, at in enumerate(spans):
            live = positions < lengths_row[:, b : b + 1]
            scores = jnp.where(live, score_buf[at, :] * scaling, NEGATIVE)
            top = jnp.max(scores, axis=1, keepdims=True)
            weights = jnp.where(live, jnp.exp(scores - top), 0.0)
            top_buf[at, :] = jnp.broadcast_to(top, (slot, LANES))
            total_buf[at, :] = jnp.broadcast_to(
                jnp.sum(weights, axis=1, keepdims=True), (slot, LANES)
            )
            weight_buf[at, :] = weights.astype(jnp.bfloat16)
        for b, at in enumerate(spans):
            value = jnp.dot(
                weight_buf[at, :], cache_ref[b, :, low:width], preferred_element_type=jnp.float32
            )
            for i, tile in enumerate(mixed):
                tile[at, :] = value[:, i * LANES : (i + 1) * LANES]
        lane = lax.broadcasted_iota(jnp.int32, (requests, LANES), 1)
        tops = jnp.full((requests, LANES), NEGATIVE, jnp.float32)
        owns = jnp.full((requests, LANES), NEGATIVE, jnp.float32)
        totals = jnp.zeros((requests, LANES), jnp.float32)
        second = ROW_TILE * -(-requests // ROW_TILE)
        stack[2 * second : 2 * second + requests, :] = latent[:, low:width]
        for j in range(heads):
            pick = pl.ds(j, requests, stride=slot)
            tops = jnp.where(lane == j, top_buf[pick, :], tops)
            totals = jnp.where(lane == j, total_buf[pick, :], totals)
            owns = jnp.where(lane == j, score_own[pick, :], owns)
            value = jnp.concatenate([tile[pick, :] for tile in mixed], axis=1)
            high = value.astype(jnp.bfloat16)
            stack[0:requests, :] = high
            stack[second : second + requests, :] = (value - high.astype(jnp.float32)).astype(
                jnp.bfloat16
            )
            at = slice(j * HEAD_DIM, (j + 1) * HEAD_DIM)
            lifted = jnp.dot(stack[...], value_ref[:, at], preferred_element_type=jnp.float32)
            put_folded(
                send_ref, requests, j * HEAD_DIM,
                lifted[0:requests] + lifted[second : second + requests],
            )
            local_ref[:, at] = lifted[2 * second : 2 * second + requests]
        put_folded(send_ref, requests, q_width, tops)
        put_folded(send_ref, requests, q_width + LANES, totals)
        local_ref[:, q_width : q_width + LANES] = owns

    tall = requests * slot
    return pl.pallas_call(
        kernel,
        out_shape=(
            jax.ShapeDtypeStruct((requests * fold, send_width // fold), jnp.float32),
            jax.ShapeDtypeStruct((requests, q_width + LANES), jnp.float32),
        ),
        in_specs=[VMEM] * 6,
        out_specs=(VMEM,) * 2,
        scratch_shapes=[
            pltpu.VMEM((tall, LANES), jnp.float32),
            pltpu.VMEM((tall, LANES), jnp.float32),
            pltpu.VMEM((tall, LANES), jnp.float32),
            pltpu.VMEM((requests, width), jnp.float32),
            pltpu.VMEM((3 * round_up(requests, ROW_TILE), full), jnp.bfloat16),
            pltpu.VMEM((tall, span), jnp.float32),
            pltpu.VMEM((tall, span), jnp.bfloat16),
        ]
        + [pltpu.VMEM((tall, LANES), jnp.float32)] * (2 * full // LANES),
        compiler_params=params(5),
        cost_estimate=cost(5),
        name="attend",
    )(
        own, other, lengths, resident(cache), resident(key_up), resident(value_pad),
    )


def merge_out(own, other, local, w_out, requests):
    q_width = local.shape[1] - LANES
    heads = q_width // HEAD_DIM
    width = w_out.shape[1]
    fold = fold_of(requests, width)
    step = 512 if width % 512 == 0 else width

    def kernel(own_ref, other_ref, local_ref, w_ref, out_ref, head_buf):
        top_a = get_folded((own_ref,), requests, q_width, LANES)
        top_b = get_folded((other_ref,), requests, q_width, LANES)
        total_a = get_folded((own_ref,), requests, q_width + LANES, LANES)
        total_b = get_folded((other_ref,), requests, q_width + LANES, LANES)
        own_score = local_ref[:, q_width : q_width + LANES]
        highest = jnp.maximum(jnp.maximum(top_a, top_b), own_score)
        scale_a = jnp.exp(top_a - highest)
        scale_b = jnp.exp(top_b - highest)
        own_weight = jnp.exp(own_score - highest)
        below = total_a * scale_a + total_b * scale_b + own_weight
        scale_a = scale_a / below
        scale_b = scale_b / below
        own_weight = own_weight / below
        for j in range(heads):
            at = slice(j * HEAD_DIM, (j + 1) * HEAD_DIM)
            value = (
                get_folded((own_ref,), requests, j * HEAD_DIM, HEAD_DIM) * scale_a[:, j : j + 1]
                + get_folded((other_ref,), requests, j * HEAD_DIM, HEAD_DIM)
                * scale_b[:, j : j + 1]
                + local_ref[:, at] * own_weight[:, j : j + 1]
            )
            head_buf[:, at] = value.astype(jnp.bfloat16)
        head_out = head_buf[...]
        for at in range(0, width, step):
            put_folded(
                out_ref, requests, at,
                jnp.dot(head_out, w_ref[:, at : at + step], preferred_element_type=jnp.float32),
            )

    return pl.pallas_call(
        kernel,
        out_shape=jax.ShapeDtypeStruct((requests * fold, width // fold), jnp.float32),
        in_specs=[VMEM] * 4,
        out_specs=VMEM,
        scratch_shapes=[pltpu.VMEM((requests, q_width), jnp.bfloat16)],
        compiler_params=params(3),
        cost_estimate=cost(2),
        name="merge_out",
    )(own, other, local, resident(w_out))


def put_terms(out_ref, rows, x, parts, low, high):
    depth = x.shape[1]
    half = depth // 2 if depth % (2 * LANES) == 0 else depth
    for ref, turned, base in parts:
        count = ref.shape[1] if turned else ref.shape[0]
        first, last = max(low, base), min(high, base + count)
        for at in range(first, last, 2 * BLOCK):
            a, b = at - base, min(at + 2 * BLOCK, last) - base
            total = None
            for k in range(0, depth, half):
                piece = x[:, k : k + half]
                if turned:
                    term = jnp.dot(
                        piece, ref[k : k + half, a:b], preferred_element_type=jnp.float32
                    )
                else:
                    term = lax.dot_general(
                        piece, ref[a:b, k : k + half], NT, preferred_element_type=jnp.float32
                    )
                total = term if total is None else total + term
            put_folded(out_ref, rows, at - low, total)


def late_scratch():
    return [pltpu.SemaphoreType.DMA((LATE,)), pltpu.SemaphoreType.REGULAR]


def late_copies(table_ref, held, sems, span):
    step = round_up(-(-(span[1] - span[0]) // LATE), ROW_TILE)
    return row_copies(table_ref, held, sems, span[0], span[1], step)


def vocab_head(own, other, hidden, gain, parts, span, table, late):
    rows, depth = hidden.shape
    low, high = span
    width = round_up(high - low + LANES, 2 * LANES)
    fold = fold_of(rows, width)
    count = len(parts)

    def kernel(own_ref, other_ref, x_ref, gain_ref, *refs):
        table_ref = refs[count]
        new_ref, scaled_ref, out_ref, held, sems, gate = refs[count + 1 :]
        copies = late_copies(table_ref, held, sems, late)
        for copy in copies:
            copy.start()
        fence(gate)
        states = x_ref[...].astype(jnp.float32)
        updated = states + get_folded((own_ref, other_ref), rows, 0, depth)
        new_ref[...] = updated.astype(jnp.bfloat16)
        scaled = (updated * gain_ref[...].reshape(1, depth)).astype(jnp.bfloat16)
        scaled_ref[...] = scaled
        square = jnp.sum(updated * updated, axis=1, keepdims=True)
        used = high - low
        put_folded(out_ref, rows, used, jnp.broadcast_to(square, (rows, width - used)))
        held_parts = [(ref, True, part[2]) for ref, part in zip(refs[:count], parts)]
        put_terms(out_ref, rows, scaled, held_parts, low, high)
        for copy in copies:
            copy.wait()

    return pl.pallas_call(
        kernel,
        out_shape=(
            pltpu.VMEM((rows, depth), jnp.bfloat16),
            jax.ShapeDtypeStruct((rows, depth), jnp.bfloat16),
            jax.ShapeDtypeStruct((rows * fold, width // fold), jnp.float32),
            pltpu.VMEM((late[1] - late[0], depth), table.dtype),
        ),
        in_specs=[VMEM] * (4 + count) + [ANY],
        out_specs=(VMEM,) * 4,
        scratch_shapes=late_scratch(),
        compiler_params=params(3),
        cost_estimate=cost(4),
        name="vocab_head",
    )(own, other, hidden, gain, *[resident(part[0]) for part in parts], stored(table))


def vocab_more(scaled, parts, span):
    rows = scaled.shape[0]
    low, high = span
    width = round_up(high - low, 2 * LANES)
    fold = fold_of(rows, width)
    count = len(parts)

    def kernel(x_ref, *refs):
        out_ref = refs[count]
        used = high - low
        if used < width:
            put_folded(out_ref, rows, used, jnp.zeros((rows, width - used), jnp.float32))
        held_parts = [(ref, part[1], part[2]) for ref, part in zip(refs[:count], parts)]
        put_terms(out_ref, rows, x_ref[...], held_parts, low, high)

    return pl.pallas_call(
        kernel,
        out_shape=jax.ShapeDtypeStruct((rows * fold, width // fold), jnp.float32),
        in_specs=[VMEM] * (1 + count),
        out_specs=VMEM,
        compiler_params=params(3),
        cost_estimate=cost(6),
        name="vocab_more",
    )(scaled, *[resident(part[0]) for part in parts])


def vocab_front(pairs, spans, draft_ids, columns, features, hidden):
    rows = draft_ids.shape[0]
    count = len(pairs)
    width = pairs[0][0].shape[0] * pairs[0][0].shape[1] // rows

    def kernel(id_ref, hidden_ref, *refs):
        inputs = [refs[2 * i : 2 * i + 2] for i in range(count)]
        logit_refs, (stat_ref, hidden_out) = refs[2 * count : 3 * count], refs[3 * count :]
        hidden_out[...] = hidden_ref[...]
        square = get_folded(inputs[0], rows, width - LANES, LANES)
        inv = lax.rsqrt(square[:, 0:1] / features + EPSILON)
        row = lax.broadcasted_iota(jnp.int32, (rows, 1), 0)
        wanted = jnp.zeros((rows, 1), jnp.int32)
        for r in range(rows):
            wanted = jnp.where(row == r, id_ref[r], wanted)
        wanted = wanted - lax.axis_index("heads") * columns
        top = jnp.full((rows, 1), NEGATIVE, jnp.float32)
        picked = total = jnp.zeros((rows, 1), jnp.float32)
        for pair, (low, high), logit_ref in zip(inputs, spans, logit_refs):
            logits = get_folded(pair, rows, 0, high - low) * inv
            logit_ref[...] = logits
            column = low + lax.broadcasted_iota(jnp.int32, logits.shape, 1)
            picked = picked + jnp.sum(
                jnp.where(column == wanted, logits, 0.0), axis=1, keepdims=True
            )
            joined = jnp.maximum(top, jnp.max(logits, axis=1, keepdims=True))
            total = total * jnp.exp(top - joined) + jnp.sum(
                jnp.exp(logits - joined), axis=1, keepdims=True
            )
            top = joined
        lane = lax.broadcasted_iota(jnp.int32, (rows, LANES), 1)
        stats = jnp.where(lane == 1, total, jnp.where(lane == 2, picked, inv))
        stat_ref[0:rows, :] = jnp.where(lane == 0, top, stats)
        stat_ref[rows : 2 * rows, :] = jnp.broadcast_to(wanted, (rows, LANES)).astype(jnp.float32)

    return pl.pallas_call(
        kernel,
        out_shape=tuple(pltpu.VMEM((rows, high - low), jnp.float32) for low, high in spans)
        + (
            jax.ShapeDtypeStruct((2 * rows, LANES), jnp.float32),
            jax.ShapeDtypeStruct(hidden.shape, hidden.dtype),
        ),
        in_specs=[SMEM] + [VMEM] * (2 * count + 1),
        out_specs=(VMEM,) * (count + 2),
        compiler_params=params(4),
        cost_estimate=cost(1),
        name="vocab_front",
    )(draft_ids, resident(hidden), *[array for pair in pairs for array in pair])


def vocab_back(own, other, front_stats, span):
    rows = front_stats.shape[0] // 2
    low, high = span

    def kernel(front_ref, own_ref, other_ref, logit_ref, stat_ref):
        top_front, total_front = front_ref[0:rows, 0:1], front_ref[0:rows, 1:2]
        picked_front, inv = front_ref[0:rows, 2:3], front_ref[0:rows, 3:4]
        wanted = front_ref[rows : 2 * rows, 0:1].astype(jnp.int32)
        logits = get_folded((own_ref, other_ref), rows, 0, high - low) * inv
        logit_ref[...] = logits
        column = low + lax.broadcasted_iota(jnp.int32, logits.shape, 1)
        picked = picked_front + jnp.sum(
            jnp.where(column == wanted, logits, 0.0), axis=1, keepdims=True
        )
        top = jnp.maximum(top_front, jnp.max(logits, axis=1, keepdims=True))
        total = total_front * jnp.exp(top_front - top) + jnp.sum(
            jnp.exp(logits - top), axis=1, keepdims=True
        )
        lane = lax.broadcasted_iota(jnp.int32, (rows, LANES), 1)
        stat_ref[...] = jnp.where(
            lane == 0, top, jnp.where(lane == 1, total, jnp.where(lane == 2, picked, 0.0))
        )

    return pl.pallas_call(
        kernel,
        out_shape=(
            pltpu.VMEM((rows, high - low), jnp.float32),
            jax.ShapeDtypeStruct((rows, LANES), jnp.float32),
        ),
        in_specs=[VMEM] * 3,
        out_specs=(VMEM, VMEM),
        compiler_params=params(4),
        cost_estimate=cost(1),
        name="vocab_back",
    )(front_stats, own, other)


def vocab_finish(pieces, spans, stats):
    rows = pieces[0].shape[0]
    columns = sum(high - low for low, high in spans)
    count = len(pieces)

    def kernel(*refs):
        piece_refs, stat_refs = refs[:count], refs[count:-2]
        out_ref, draft_ref = refs[-2:]
        state = [(ref[:, 0:1], ref[:, 1:2], ref[:, 2:3]) for ref in stat_refs]
        while len(state) > 1:
            joined = []
            for (top_a, sum_a, pick_a), (top_b, sum_b, pick_b) in zip(state[0::2], state[1::2]):
                top = jnp.maximum(top_a, top_b)
                joined.append(
                    (
                        top,
                        sum_a * jnp.exp(top_a - top) + sum_b * jnp.exp(top_b - top),
                        pick_a + pick_b,
                    )
                )
            state = joined
        top, total, picked = state[0]
        log_total = top + jnp.log(total)
        for ref, (low, high) in zip(piece_refs, spans):
            out_ref[:, low:high] = ref[...] - log_total
        draft = picked - log_total
        row = lax.broadcasted_iota(jnp.int32, (rows, LANES), 0)
        lane = lax.broadcasted_iota(jnp.int32, (rows, LANES), 1)
        line = jnp.sum(jnp.where(row == lane, draft, 0.0), axis=0, keepdims=True)
        draft_ref[...] = line[:, 0:rows]

    return pl.pallas_call(
        kernel,
        out_shape=(
            jax.ShapeDtypeStruct((rows, columns), jnp.float32),
            jax.ShapeDtypeStruct((1, rows), jnp.float32),
        ),
        in_specs=[VMEM] * (count + len(stats)),
        out_specs=(VMEM, VMEM),
        compiler_params=params(4),
        cost_estimate=cost(1),
        name="vocab_finish",
    )(*[resident(piece) for piece in pieces], *stats)


def pair_sum(array, axis):
    if lax.axis_size(axis) == 2:
        return array, swap(array, axis, 1)
    return lax.psum(array, axis), jnp.zeros_like(array)


def pair_softmax(array, axis, requests, q_width):
    if lax.axis_size(axis) == 2:
        return array, swap(array, axis, 1)
    fold = array.shape[0] // requests
    width = array.shape[1]
    flat = jnp.concatenate(
        [array[i * requests : (i + 1) * requests] for i in range(fold)], axis=1
    )
    every = lax.all_gather(flat, axis)
    tops = every[:, :, q_width : q_width + LANES]
    totals = every[:, :, q_width + LANES :]
    top = jnp.max(tops, axis=0)
    scale = jnp.exp(tops - top)
    heads = q_width // HEAD_DIM
    total = jnp.sum(totals * scale, axis=0)
    mixed = every[:, :, :q_width].reshape(every.shape[0], requests, heads, HEAD_DIM)
    mixed = jnp.sum(mixed * scale[:, :, :heads, None], axis=0).reshape(requests, q_width)
    flat = jnp.concatenate([mixed, top, total], axis=1)
    empty = jnp.concatenate(
        [jnp.zeros_like(mixed), jnp.full_like(top, NEGATIVE), jnp.zeros_like(total)], axis=1
    )

    def folded(value):
        return jnp.concatenate(
            [value[:, i * width : (i + 1) * width] for i in range(fold)], axis=0
        )

    return folded(flat), folded(empty)


def body(
    hidden_in,
    lengths,
    draft_ids,
    input_gain,
    w_query,
    w_latent,
    latent_cache,
    key_up,
    value_up,
    w_out,
    final_gain,
    w_vocab,
):
    rows, depth = hidden_in.shape
    features = depth * lax.axis_size("seq")
    columns = w_vocab.shape[1]
    table = w_vocab.T
    q_width = w_query.shape[1]

    def mark(share):
        return int(columns * share) // BLOCK * BLOCK

    marks = [mark(0.16), mark(0.256), mark(0.352), mark(0.576), columns]
    spans = [(mark(0.544), columns), (0, mark(0.544))]

    sums = project(
        hidden_in,
        input_gain,
        w_query,
        w_latent.reshape(depth, w_latent.shape[1] * w_latent.shape[2]),
    )
    own, other = pair_sum(sums, "seq")
    cache, keys, values, turned = fetch_attention(
        latent_cache[:, 0], key_up[0], value_up[0], table, sums, marks[0], marks[1], 3
    )
    turned = [turned]
    packed, local = attend(
        own, other, lengths, cache, keys, values, features
    )
    own, other = pair_softmax(packed, "seq", rows, q_width)
    turned.append(fetch_turned(table, packed, marks[1], marks[2], 3))
    part = merge_out(own, other, local, w_out, rows)

    heads = lax.axis_size("heads")
    first = part
    if is_power(heads) and heads > 1:
        mask = 1
        while True:
            received = swap(part, "heads", mask)
            mask *= 2
            if mask >= heads:
                break
            part = part + received
    else:
        part, received = lax.psum(part, "heads"), jnp.zeros_like(part)
    turned.append(fetch_turned(table, first, marks[2], marks[3], 3))
    turned.append(fetch_turned(table, part, marks[3], marks[4], 6))

    parts = [(part_, True, low) for part_, low in zip(turned, marks)]
    updated, scaled, piece, late_part = vocab_head(
        part, received, hidden_in, final_gain, parts, spans[0], table, (0, marks[0])
    )
    pairs = [pair_sum(piece, "seq")]
    piece = vocab_more(scaled, parts + [(late_part, False, 0)], spans[1])
    own, other = pair_sum(piece, "seq")
    *logits, front_stats, new_hidden = vocab_front(
        pairs, spans[:1], draft_ids, columns, features, updated
    )
    back, stats = vocab_back(own, other, front_stats, spans[1])
    if is_power(heads):
        every = [stats]
        for mask in range(1, heads):
            every.append(swap(stats, "heads", mask))
    else:
        gathered = lax.all_gather(stats, "heads")
        every = [gathered[i] for i in range(heads)]
        while not is_power(len(every)):
            every.append(jnp.concatenate([jnp.full_like(stats[:, :1], NEGATIVE), jnp.zeros_like(stats[:, 1:])], axis=1))
    log_probs, draft = vocab_finish(logits + [back], spans, every)
    return (new_hidden, log_probs, draft.reshape(rows))


def solution(mesh):
    return jax.shard_map(
        body,
        mesh=mesh,
        in_specs=(
            P("batch", "seq"),
            P("batch"),
            P("batch"),
            P("seq"),
            P("seq", "heads"),
            P("seq", "heads", None),
            P("batch", "heads", "seq", None),
            P("heads", None, None),
            P("heads", None, None),
            P("heads", "seq"),
            P("seq"),
            P("seq", "heads"),
        ),
        out_specs=(P("batch", "seq"), P("batch", "heads"), P("batch")),
        check_vma=False,
    )
```

```python
import math

import jax
import jax.numpy as jnp
from jax import lax
from jax.experimental import pallas as pl
from jax.experimental.pallas import tpu as pltpu
from jax.sharding import PartitionSpec as P


HEAD_DIM = 128
LANES = 128
ROW_TILE = 16
BLOCK = 256
RING = 7
LATE = 2
EPSILON = 1e-05
NEGATIVE = -1e30
MIB = 1 << 20
ANY = pl.BlockSpec(memory_space=pl.ANY)
VMEM = pl.BlockSpec(memory_space=pltpu.VMEM)
SMEM = pl.BlockSpec(memory_space=pltpu.SMEM)
NT = (((1,), (1,)), ((), ()))


def resident(array):
    return pltpu.with_memory_space_constraint(array, pltpu.VMEM)


def stored(array):
    return pltpu.with_memory_space_constraint(array, pltpu.HBM)


def cost(micros):
    return pl.CostEstimate(flops=int(micros * 5e6), bytes_accessed=0, transcendentals=0)


def params(mib):
    return pltpu.CompilerParams(vmem_limit_bytes=int(mib * MIB))


def round_up(value, step):
    return -(-value // step) * step


def fold_of(rows, width):
    fold = 8 // math.gcd(rows, 8)
    return fold if width % (fold * LANES) == 0 else 1


def put_folded(ref, rows, start, value):
    width = ref.shape[1]
    done = 0
    while done < value.shape[1]:
        piece, at = divmod(start + done, width)
        size = min(value.shape[1] - done, width - at)
        ref[piece * rows : (piece + 1) * rows, at : at + size] = value[:, done : done + size]
        done += size


def get_folded(refs, rows, start, size):
    width = refs[0].shape[1]
    pieces = []
    done = 0
    while done < size:
        piece, at = divmod(start + done, width)
        span = min(size - done, width - at)
        block = None
        for ref in refs:
            term = ref[piece * rows : (piece + 1) * rows, at : at + span]
            block = term if block is None else block + term
        pieces.append(block)
        done += span
    return pieces[0] if len(pieces) == 1 else jnp.concatenate(pieces, axis=1)


def swap(array, axis, mask):
    size = lax.axis_size(axis)
    return lax.ppermute(array, axis, [(i, i ^ mask) for i in range(size)])


def fence(sem):
    pl.semaphore_signal(sem, 1)
    pl.semaphore_wait(sem, 1)


def is_power(size):
    return size & (size - 1) == 0


def project(hidden, gain, w_query, w_latent):
    rows, depth = hidden.shape
    q_width, l_width = w_query.shape[1], w_latent.shape[1]
    width = q_width + l_width + LANES
    fold = fold_of(rows, width)
    chunks = 5 if depth % (5 * LANES) == 0 else 1
    spans = [(depth * i // chunks, depth * (i + 1) // chunks) for i in range(chunks)]

    def kernel(x_hbm, gain_hbm, wq_ref, wl_ref, out_ref, x_ref, gain_ref, q_buf, l_buf, sems, ends, gate):
        small = [
            pltpu.make_async_copy(x_hbm, x_ref, ends.at[0]),
            pltpu.make_async_copy(gain_hbm, gain_ref, ends.at[1]),
        ]
        for copy in small:
            copy.start()
        fence(gate)
        copies = []
        for c, (a, b) in enumerate(spans):
            at = pl.ds(a, b - a)
            copies.append(
                (
                    pltpu.make_async_copy(wq_ref.at[at], q_buf.at[at], sems.at[0, c]),
                    pltpu.make_async_copy(wl_ref.at[at], l_buf.at[at], sems.at[1, c]),
                )
            )
        for pair in copies:
            for copy in pair:
                copy.start()
        for copy in small:
            copy.wait()
        states = x_ref[...].astype(jnp.float32)
        gained = (states * gain_ref[...].reshape(1, depth)).astype(jnp.bfloat16)
        square = jnp.sum(states * states, axis=1, keepdims=True)
        acc_q = acc_l = None
        for c, (a, b) in enumerate(spans):
            for copy in copies[c]:
                copy.wait()
            x = gained[:, a:b]
            part_q = jnp.dot(x, q_buf[a:b, :], preferred_element_type=jnp.float32)
            part_l = jnp.dot(x, l_buf[a:b, :], preferred_element_type=jnp.float32)
            acc_q = part_q if c == 0 else acc_q + part_q
            acc_l = part_l if c == 0 else acc_l + part_l
        put_folded(out_ref, rows, 0, acc_q)
        put_folded(out_ref, rows, q_width, acc_l)
        put_folded(out_ref, rows, q_width + l_width, jnp.broadcast_to(square, (rows, LANES)))

    return pl.pallas_call(
        kernel,
        out_shape=jax.ShapeDtypeStruct((rows * fold, width // fold), jnp.float32),
        in_specs=[ANY] * 4,
        out_specs=VMEM,
        scratch_shapes=[
            pltpu.VMEM(hidden.shape, hidden.dtype),
            pltpu.VMEM(gain.shape, gain.dtype),
            pltpu.VMEM(w_query.shape, w_query.dtype),
            pltpu.VMEM(w_latent.shape, w_latent.dtype),
            pltpu.SemaphoreType.DMA((2, chunks)),
            pltpu.SemaphoreType.DMA((2,)),
            pltpu.SemaphoreType.REGULAR,
        ],
        compiler_params=params(14),
        cost_estimate=cost(5),
        name="project",
    )(stored(hidden), stored(gain), stored(w_query), stored(w_latent))


def row_copies(table_ref, out_ref, sems, low, high, step):
    bounds = [(at, min(at + step, high)) for at in range(low, high, step)]
    return [
        pltpu.make_async_copy(
            table_ref.at[pl.ds(a, b - a)], out_ref.at[pl.ds(a - low, b - a)], sems.at[i]
        )
        for i, (a, b) in enumerate(bounds)
    ]


def turn_copies(table_ref, held_ref, sems, low, high):
    slots = held_ref.shape[0]
    copies = []
    for i, at in enumerate(range(low, high, BLOCK)):
        size = min(BLOCK, high - at)
        copies.append(
            pltpu.make_async_copy(
                table_ref.at[pl.ds(at, size)],
                held_ref.at[i % slots, pl.ds(0, size)],
                sems.at[i % slots],
            )
        )
    return copies


def turn_rows(copies, held_ref, out_ref):
    slots, _, depth = held_ref.shape
    count = out_ref.shape[1]
    one = lax.broadcasted_iota(jnp.int32, (BLOCK, BLOCK), 0)
    one = (one == lax.broadcasted_iota(jnp.int32, (BLOCK, BLOCK), 1)).astype(out_ref.dtype)
    for i, copy in enumerate(copies):
        copy.wait()
        a, b = i * BLOCK, min((i + 1) * BLOCK, count)
        for k in range(0, depth, BLOCK):
            end = min(k + BLOCK, depth)
            tile = held_ref[i % slots, 0 : b - a, k:end]
            if k // BLOCK % 3 == 1 and end - k == BLOCK:
                tile = lax.dot_general(one, tile, NT, preferred_element_type=jnp.float32)
                out_ref[k:end, a:b] = tile.astype(out_ref.dtype)
            else:
                out_ref[k:end, a:b] = tile.T
        if i + slots < len(copies):
            copies[i + slots].start()


def turn_slots(count):
    return min(RING, -(-count // BLOCK))


def turn_scratch(table, count):
    return [
        pltpu.VMEM((turn_slots(count), BLOCK, table.shape[1]), table.dtype),
        pltpu.SemaphoreType.DMA((turn_slots(count),)),
    ]


def turn_params(table, count):
    size = turn_slots(count) * BLOCK * round_up(table.shape[1], LANES) * 2
    return params(1 + size / MIB)


def fetch_turned(table, after, low, high, micros):
    def kernel(table_ref, after_ref, out_ref, held, sems):
        copies = turn_copies(table_ref, held, sems, low, high)
        for copy in copies[: held.shape[0]]:
            copy.start()
        turn_rows(copies, held, out_ref)

    return pl.pallas_call(
        kernel,
        out_shape=pltpu.VMEM((table.shape[1], high - low), table.dtype),
        in_specs=[ANY, ANY],
        out_specs=VMEM,
        scratch_shapes=turn_scratch(table, high - low),
        compiler_params=turn_params(table, high - low),
        cost_estimate=cost(micros),
        name="fetch_turned",
    )(stored(table), after)


def fetch_attention(cache, key_up, value_up, table, after, low, high, micros):
    rank, width = value_up.shape
    full = round_up(rank, LANES)

    def kernel(
        cache_ref, key_ref, value_ref, table_ref, after_ref,
        cache_out, key_out, value_out, turned_out, sems, held, row_sems,
    ):
        copies = [
            pltpu.make_async_copy(key_ref, key_out, sems.at[0]),
            pltpu.make_async_copy(value_ref, value_out.at[pl.ds(full - rank, rank)], sems.at[1]),
            pltpu.make_async_copy(cache_ref, cache_out, sems.at[2]),
        ]
        rows = turn_copies(table_ref, held, row_sems, low, high)
        for copy in rows[: held.shape[0]] + copies:
            copy.start()
        value_out[0 : full - rank, :] = jnp.zeros((full - rank, width), value_up.dtype)
        turn_rows(rows, held, turned_out)
        for copy in copies:
            copy.wait()

    return pl.pallas_call(
        kernel,
        out_shape=(
            pltpu.VMEM(cache.shape, cache.dtype),
            pltpu.VMEM(key_up.shape, key_up.dtype),
            pltpu.VMEM((full, width), value_up.dtype),
            pltpu.VMEM((table.shape[1], high - low), table.dtype),
        ),
        in_specs=[ANY] * 5,
        out_specs=(VMEM,) * 4,
        scratch_shapes=[pltpu.SemaphoreType.DMA((3,))] + turn_scratch(table, high - low),
        compiler_params=turn_params(table, high - low),
        cost_estimate=cost(micros),
        name="fetch_attention",
    )(stored(cache), stored(key_up), stored(value_up), stored(table), after)


def attend(own, other, lengths, cache, key_up, value_pad, features):
    requests, span, width = cache.shape
    rank = width // 2
    full = value_pad.shape[0]
    low = width - full
    heads = key_up.shape[1] // HEAD_DIM
    slot = round_up(heads, ROW_TILE)
    scaling = 1.0 / math.sqrt(HEAD_DIM)
    q_width = heads * HEAD_DIM
    send_width = q_width + 2 * LANES
    fold = fold_of(requests, send_width)

    def kernel(
        own_ref, other_ref, length_ref, cache_ref, key_ref, value_ref,
        send_ref, local_ref, score_own, top_buf, total_buf, latent_buf, stack,
        score_buf, weight_buf, *tiles,
    ):
        absorbed, mixed = tiles[: full // LANES], tiles[full // LANES :]
        refs = (own_ref, other_ref)
        square = get_folded(refs, requests, q_width + width, LANES)
        inv = lax.rsqrt(square[:, 0:1] / features + EPSILON)
        query = (inv * get_folded(refs, requests, 0, q_width)).astype(jnp.bfloat16)
        latent = (inv * get_folded(refs, requests, q_width, width)).astype(jnp.bfloat16)
        latent_buf[...] = latent.astype(jnp.float32)
        for tile in absorbed:
            tile[...] = jnp.zeros(tile.shape, jnp.float32)
        for j in range(heads):
            at = slice(j * HEAD_DIM, (j + 1) * HEAD_DIM)
            row = lax.dot_general(
                query[:, at], key_ref[:, at], NT, preferred_element_type=jnp.float32
            )
            row = row.astype(jnp.bfloat16).astype(jnp.float32)
            for i, tile in enumerate(absorbed):
                piece = row[:, i * LANES : min((i + 1) * LANES, rank)]
                if piece.shape[1] < LANES:
                    edge = jnp.zeros((requests, LANES - piece.shape[1]), jnp.float32)
                    piece = jnp.concatenate([piece, edge], axis=1)
                tile[pl.ds(j, requests, stride=slot), :] = piece
        first = lax.axis_index("seq") * span
        positions = first + lax.broadcasted_iota(jnp.int32, (slot, span), 1)
        spans = [slice(b * slot, (b + 1) * slot) for b in range(requests)]
        for b, at in enumerate(spans):
            rows = jnp.concatenate([tile[at, :] for tile in absorbed], axis=1)
            score_buf[at, :] = lax.dot_general(
                rows.astype(jnp.bfloat16),
                cache_ref[b, :, 0:full],
                NT,
                preferred_element_type=jnp.float32,
            )
            score_own[at, :] = jnp.broadcast_to(
                jnp.sum(rows * latent_buf[b : b + 1, 0:full], axis=1, keepdims=True) * scaling,
                (slot, LANES),
            )
        lengths_row = length_ref[...].reshape(1, requests)
        for b, at in enumerate(spans):
            live = positions < lengths_row[:, b : b + 1]
            scores = jnp.where(live, score_buf[at, :] * scaling, NEGATIVE)
            top = jnp.max(scores, axis=1, keepdims=True)
            weights = jnp.where(live, jnp.exp(scores - top), 0.0)
            top_buf[at, :] = jnp.broadcast_to(top, (slot, LANES))
            total_buf[at, :] = jnp.broadcast_to(
                jnp.sum(weights, axis=1, keepdims=True), (slot, LANES)
            )
            weight_buf[at, :] = weights.astype(jnp.bfloat16)
        for b, at in enumerate(spans):
            value = jnp.dot(
                weight_buf[at, :], cache_ref[b, :, low:width], preferred_element_type=jnp.float32
            )
            for i, tile in enumerate(mixed):
                tile[at, :] = value[:, i * LANES : (i + 1) * LANES]
        lane = lax.broadcasted_iota(jnp.int32, (requests, LANES), 1)
        tops = jnp.full((requests, LANES), NEGATIVE, jnp.float32)
        owns = jnp.full((requests, LANES), NEGATIVE, jnp.float32)
        totals = jnp.zeros((requests, LANES), jnp.float32)
        second = ROW_TILE * -(-requests // ROW_TILE)
        stack[2 * second : 2 * second + requests, :] = latent[:, low:width]
        for j in range(heads):
            pick = pl.ds(j, requests, stride=slot)
            tops = jnp.where(lane == j, top_buf[pick, :], tops)
            totals = jnp.where(lane == j, total_buf[pick, :], totals)
            owns = jnp.where(lane == j, score_own[pick, :], owns)
            value = jnp.concatenate([tile[pick, :] for tile in mixed], axis=1)
            high = value.astype(jnp.bfloat16)
            stack[0:requests, :] = high
            stack[second : second + requests, :] = (value - high.astype(jnp.float32)).astype(
                jnp.bfloat16
            )
            at = slice(j * HEAD_DIM, (j + 1) * HEAD_DIM)
            lifted = jnp.dot(stack[...], value_ref[:, at], preferred_element_type=jnp.float32)
            put_folded(
                send_ref, requests, j * HEAD_DIM,
                lifted[0:requests] + lifted[second : second + requests],
            )
            local_ref[:, at] = lifted[2 * second : 2 * second + requests]
        put_folded(send_ref, requests, q_width, tops)
        put_folded(send_ref, requests, q_width + LANES, totals)
        local_ref[:, q_width : q_width + LANES] = owns

    tall = round_up(requests, 8) * slot
    return pl.pallas_call(
        kernel,
        out_shape=(
            jax.ShapeDtypeStruct((requests * fold, send_width // fold), jnp.float32),
            jax.ShapeDtypeStruct((requests, q_width + LANES), jnp.float32),
        ),
        in_specs=[VMEM] * 6,
        out_specs=(VMEM,) * 2,
        scratch_shapes=[
            pltpu.VMEM((tall, LANES), jnp.float32),
            pltpu.VMEM((tall, LANES), jnp.float32),
            pltpu.VMEM((tall, LANES), jnp.float32),
            pltpu.VMEM((requests, width), jnp.float32),
            pltpu.VMEM((3 * round_up(requests, ROW_TILE), full), jnp.bfloat16),
            pltpu.VMEM((tall, span), jnp.float32),
            pltpu.VMEM((tall, span), jnp.bfloat16),
        ]
        + [pltpu.VMEM((tall, LANES), jnp.float32)] * (2 * full // LANES),
        compiler_params=params(5),
        cost_estimate=cost(5),
        name="attend",
    )(
        own, other, lengths, resident(cache), resident(key_up), resident(value_pad),
    )


def merge_out(own, other, local, w_out, requests):
    q_width = local.shape[1] - LANES
    heads = q_width // HEAD_DIM
    width = w_out.shape[1]
    fold = fold_of(requests, width)
    step = 512 if width % 512 == 0 else width

    def kernel(own_ref, other_ref, local_ref, w_ref, out_ref, head_buf):
        top_a = get_folded((own_ref,), requests, q_width, LANES)
        top_b = get_folded((other_ref,), requests, q_width, LANES)
        total_a = get_folded((own_ref,), requests, q_width + LANES, LANES)
        total_b = get_folded((other_ref,), requests, q_width + LANES, LANES)
        own_score = local_ref[:, q_width : q_width + LANES]
        highest = jnp.maximum(jnp.maximum(top_a, top_b), own_score)
        scale_a = jnp.exp(top_a - highest)
        scale_b = jnp.exp(top_b - highest)
        own_weight = jnp.exp(own_score - highest)
        below = total_a * scale_a + total_b * scale_b + own_weight
        scale_a = scale_a / below
        scale_b = scale_b / below
        own_weight = own_weight / below
        for j in range(heads):
            at = slice(j * HEAD_DIM, (j + 1) * HEAD_DIM)
            value = (
                get_folded((own_ref,), requests, j * HEAD_DIM, HEAD_DIM) * scale_a[:, j : j + 1]
                + get_folded((other_ref,), requests, j * HEAD_DIM, HEAD_DIM)
                * scale_b[:, j : j + 1]
                + local_ref[:, at] * own_weight[:, j : j + 1]
            )
            head_buf[:, at] = value.astype(jnp.bfloat16)
        head_out = head_buf[...]
        for at in range(0, width, step):
            put_folded(
                out_ref, requests, at,
                jnp.dot(head_out, w_ref[:, at : at + step], preferred_element_type=jnp.float32),
            )

    return pl.pallas_call(
        kernel,
        out_shape=jax.ShapeDtypeStruct((requests * fold, width // fold), jnp.float32),
        in_specs=[VMEM] * 4,
        out_specs=VMEM,
        scratch_shapes=[pltpu.VMEM((requests, q_width), jnp.bfloat16)],
        compiler_params=params(3),
        cost_estimate=cost(2),
        name="merge_out",
    )(own, other, local, resident(w_out))


def put_terms(out_ref, rows, x, parts, low, high):
    depth = x.shape[1]
    half = depth // 2 if depth % (2 * LANES) == 0 else depth
    for ref, turned, base in parts:
        count = ref.shape[1] if turned else ref.shape[0]
        first, last = max(low, base), min(high, base + count)
        for at in range(first, last, 2 * BLOCK):
            a, b = at - base, min(at + 2 * BLOCK, last) - base
            total = None
            for k in range(0, depth, half):
                piece = x[:, k : k + half]
                if turned:
                    term = jnp.dot(
                        piece, ref[k : k + half, a:b], preferred_element_type=jnp.float32
                    )
                else:
                    term = lax.dot_general(
                        piece, ref[a:b, k : k + half], NT, preferred_element_type=jnp.float32
                    )
                total = term if total is None else total + term
            put_folded(out_ref, rows, at - low, total)


def late_scratch():
    return [pltpu.SemaphoreType.DMA((LATE,)), pltpu.SemaphoreType.REGULAR]


def late_copies(table_ref, held, sems, span):
    step = round_up(-(-(span[1] - span[0]) // LATE), ROW_TILE)
    return row_copies(table_ref, held, sems, span[0], span[1], step)


def vocab_head(own, other, hidden, gain, parts, span, table, late):
    rows, depth = hidden.shape
    low, high = span
    width = round_up(high - low + LANES, 2 * LANES)
    fold = fold_of(rows, width)
    count = len(parts)

    def kernel(own_ref, other_ref, x_ref, gain_ref, *refs):
        table_ref = refs[count]
        new_ref, scaled_ref, out_ref, held, sems, gate = refs[count + 1 :]
        copies = late_copies(table_ref, held, sems, late)
        for copy in copies:
            copy.start()
        fence(gate)
        states = x_ref[...].astype(jnp.float32)
        updated = states + get_folded((own_ref, other_ref), rows, 0, depth)
        new_ref[...] = updated.astype(jnp.bfloat16)
        scaled = (updated * gain_ref[...].reshape(1, depth)).astype(jnp.bfloat16)
        scaled_ref[...] = scaled
        square = jnp.sum(updated * updated, axis=1, keepdims=True)
        used = high - low
        put_folded(out_ref, rows, used, jnp.broadcast_to(square, (rows, width - used)))
        held_parts = [(ref, True, part[2]) for ref, part in zip(refs[:count], parts)]
        put_terms(out_ref, rows, scaled, held_parts, low, high)
        for copy in copies:
            copy.wait()

    return pl.pallas_call(
        kernel,
        out_shape=(
            pltpu.VMEM((rows, depth), jnp.bfloat16),
            jax.ShapeDtypeStruct((rows, depth), jnp.bfloat16),
            jax.ShapeDtypeStruct((rows * fold, width // fold), jnp.float32),
            pltpu.VMEM((late[1] - late[0], depth), table.dtype),
        ),
        in_specs=[VMEM] * (4 + count) + [ANY],
        out_specs=(VMEM,) * 4,
        scratch_shapes=late_scratch(),
        compiler_params=params(3),
        cost_estimate=cost(4),
        name="vocab_head",
    )(own, other, hidden, gain, *[resident(part[0]) for part in parts], stored(table))


def vocab_more(scaled, parts, span):
    rows = scaled.shape[0]
    low, high = span
    width = round_up(high - low, 2 * LANES)
    fold = fold_of(rows, width)
    count = len(parts)

    def kernel(x_ref, *refs):
        out_ref = refs[count]
        used = high - low
        if used < width:
            put_folded(out_ref, rows, used, jnp.zeros((rows, width - used), jnp.float32))
        held_parts = [(ref, part[1], part[2]) for ref, part in zip(refs[:count], parts)]
        put_terms(out_ref, rows, x_ref[...], held_parts, low, high)

    return pl.pallas_call(
        kernel,
        out_shape=jax.ShapeDtypeStruct((rows * fold, width // fold), jnp.float32),
        in_specs=[VMEM] * (1 + count),
        out_specs=VMEM,
        compiler_params=params(3),
        cost_estimate=cost(6),
        name="vocab_more",
    )(scaled, *[resident(part[0]) for part in parts])


def vocab_front(pairs, spans, draft_ids, columns, features, hidden):
    rows = draft_ids.shape[0]
    count = len(pairs)
    width = pairs[0][0].shape[0] * pairs[0][0].shape[1] // rows

    def kernel(id_ref, hidden_ref, *refs):
        inputs = [refs[2 * i : 2 * i + 2] for i in range(count)]
        logit_refs, (stat_ref, hidden_out) = refs[2 * count : 3 * count], refs[3 * count :]
        hidden_out[...] = hidden_ref[...]
        square = get_folded(inputs[0], rows, width - LANES, LANES)
        inv = lax.rsqrt(square[:, 0:1] / features + EPSILON)
        row = lax.broadcasted_iota(jnp.int32, (rows, 1), 0)
        wanted = jnp.zeros((rows, 1), jnp.int32)
        for r in range(rows):
            wanted = jnp.where(row == r, id_ref[r], wanted)
        wanted = wanted - lax.axis_index("heads") * columns
        top = jnp.full((rows, 1), NEGATIVE, jnp.float32)
        picked = total = jnp.zeros((rows, 1), jnp.float32)
        for pair, (low, high), logit_ref in zip(inputs, spans, logit_refs):
            logits = get_folded(pair, rows, 0, high - low) * inv
            logit_ref[...] = logits
            column = low + lax.broadcasted_iota(jnp.int32, logits.shape, 1)
            picked = picked + jnp.sum(
                jnp.where(column == wanted, logits, 0.0), axis=1, keepdims=True
            )
            joined = jnp.maximum(top, jnp.max(logits, axis=1, keepdims=True))
            total = total * jnp.exp(top - joined) + jnp.sum(
                jnp.exp(logits - joined), axis=1, keepdims=True
            )
            top = joined
        lane = lax.broadcasted_iota(jnp.int32, (rows, LANES), 1)
        stats = jnp.where(lane == 1, total, jnp.where(lane == 2, picked, inv))
        stat_ref[0:rows, :] = jnp.where(lane == 0, top, stats)
        stat_ref[rows : 2 * rows, :] = jnp.broadcast_to(wanted, (rows, LANES)).astype(jnp.float32)

    return pl.pallas_call(
        kernel,
        out_shape=tuple(pltpu.VMEM((rows, high - low), jnp.float32) for low, high in spans)
        + (
            jax.ShapeDtypeStruct((2 * rows, LANES), jnp.float32),
            jax.ShapeDtypeStruct(hidden.shape, hidden.dtype),
        ),
        in_specs=[SMEM] + [VMEM] * (2 * count + 1),
        out_specs=(VMEM,) * (count + 2),
        compiler_params=params(4),
        cost_estimate=cost(1),
        name="vocab_front",
    )(draft_ids, resident(hidden), *[array for pair in pairs for array in pair])


def vocab_back(own, other, front_stats, span):
    rows = front_stats.shape[0] // 2
    low, high = span

    def kernel(front_ref, own_ref, other_ref, logit_ref, stat_ref):
        top_front, total_front = front_ref[0:rows, 0:1], front_ref[0:rows, 1:2]
        picked_front, inv = front_ref[0:rows, 2:3], front_ref[0:rows, 3:4]
        wanted = front_ref[rows : 2 * rows, 0:1].astype(jnp.int32)
        logits = get_folded((own_ref, other_ref), rows, 0, high - low) * inv
        logit_ref[...] = logits
        column = low + lax.broadcasted_iota(jnp.int32, logits.shape, 1)
        picked = picked_front + jnp.sum(
            jnp.where(column == wanted, logits, 0.0), axis=1, keepdims=True
        )
        top = jnp.maximum(top_front, jnp.max(logits, axis=1, keepdims=True))
        total = total_front * jnp.exp(top_front - top) + jnp.sum(
            jnp.exp(logits - top), axis=1, keepdims=True
        )
        lane = lax.broadcasted_iota(jnp.int32, (rows, LANES), 1)
        stat_ref[...] = jnp.where(
            lane == 0, top, jnp.where(lane == 1, total, jnp.where(lane == 2, picked, 0.0))
        )

    return pl.pallas_call(
        kernel,
        out_shape=(
            pltpu.VMEM((rows, high - low), jnp.float32),
            jax.ShapeDtypeStruct((rows, LANES), jnp.float32),
        ),
        in_specs=[VMEM] * 3,
        out_specs=(VMEM, VMEM),
        compiler_params=params(4),
        cost_estimate=cost(1),
        name="vocab_back",
    )(front_stats, own, other)


def vocab_finish(pieces, spans, stats):
    rows = pieces[0].shape[0]
    columns = sum(high - low for low, high in spans)
    count = len(pieces)

    def kernel(*refs):
        piece_refs, stat_refs = refs[:count], refs[count:-2]
        out_ref, draft_ref = refs[-2:]
        state = [(ref[:, 0:1], ref[:, 1:2], ref[:, 2:3]) for ref in stat_refs]
        while len(state) > 1:
            joined = []
            for (top_a, sum_a, pick_a), (top_b, sum_b, pick_b) in zip(state[0::2], state[1::2]):
                top = jnp.maximum(top_a, top_b)
                joined.append(
                    (
                        top,
                        sum_a * jnp.exp(top_a - top) + sum_b * jnp.exp(top_b - top),
                        pick_a + pick_b,
                    )
                )
            state = joined
        top, total, picked = state[0]
        log_total = top + jnp.log(total)
        for ref, (low, high) in zip(piece_refs, spans):
            out_ref[:, low:high] = ref[...] - log_total
        draft = picked - log_total
        row = lax.broadcasted_iota(jnp.int32, (rows, LANES), 0)
        lane = lax.broadcasted_iota(jnp.int32, (rows, LANES), 1)
        line = jnp.sum(jnp.where(row == lane, draft, 0.0), axis=0, keepdims=True)
        draft_ref[...] = line[:, 0:rows]

    return pl.pallas_call(
        kernel,
        out_shape=(
            jax.ShapeDtypeStruct((rows, columns), jnp.float32),
            jax.ShapeDtypeStruct((1, rows), jnp.float32),
        ),
        in_specs=[VMEM] * (count + len(stats)),
        out_specs=(VMEM, VMEM),
        compiler_params=params(4),
        cost_estimate=cost(1),
        name="vocab_finish",
    )(*[resident(piece) for piece in pieces], *stats)


def pair_sum(array, axis):
    if lax.axis_size(axis) == 2:
        return array, swap(array, axis, 1)
    return lax.psum(array, axis), jnp.zeros_like(array)


def pair_softmax(array, axis, requests, q_width):
    if lax.axis_size(axis) == 2:
        return array, swap(array, axis, 1)
    fold = array.shape[0] // requests
    width = array.shape[1]
    flat = jnp.concatenate(
        [array[i * requests : (i + 1) * requests] for i in range(fold)], axis=1
    )
    every = lax.all_gather(flat, axis)
    tops = every[:, :, q_width : q_width + LANES]
    totals = every[:, :, q_width + LANES :]
    top = jnp.max(tops, axis=0)
    scale = jnp.exp(tops - top)
    heads = q_width // HEAD_DIM
    total = jnp.sum(totals * scale, axis=0)
    mixed = every[:, :, :q_width].reshape(every.shape[0], requests, heads, HEAD_DIM)
    mixed = jnp.sum(mixed * scale[:, :, :heads, None], axis=0).reshape(requests, q_width)
    flat = jnp.concatenate([mixed, top, total], axis=1)
    empty = jnp.concatenate(
        [jnp.zeros_like(mixed), jnp.full_like(top, NEGATIVE), jnp.zeros_like(total)], axis=1
    )

    def folded(value):
        return jnp.concatenate(
            [value[:, i * width : (i + 1) * width] for i in range(fold)], axis=0
        )

    return folded(flat), folded(empty)


def body(
    hidden_in,
    lengths,
    draft_ids,
    input_gain,
    w_query,
    w_latent,
    latent_cache,
    key_up,
    value_up,
    w_out,
    final_gain,
    w_vocab,
):
    rows, depth = hidden_in.shape
    features = depth * lax.axis_size("seq")
    columns = w_vocab.shape[1]
    table = w_vocab.T
    q_width = w_query.shape[1]

    def mark(share):
        return int(columns * share) // BLOCK * BLOCK

    marks = [mark(0.16), mark(0.256), mark(0.352), mark(0.592), columns]
    spans = [(mark(0.48), columns), (0, mark(0.48))]

    sums = project(
        hidden_in,
        input_gain,
        w_query,
        w_latent.reshape(depth, w_latent.shape[1] * w_latent.shape[2]),
    )
    own, other = pair_sum(sums, "seq")
    cache, keys, values, turned = fetch_attention(
        latent_cache[:, 0], key_up[0], value_up[0], table, sums, marks[0], marks[1], 3
    )
    turned = [turned]
    packed, local = attend(
        own, other, lengths, cache, keys, values, features
    )
    own, other = pair_softmax(packed, "seq", rows, q_width)
    turned.append(fetch_turned(table, packed, marks[1], marks[2], 3))
    part = merge_out(own, other, local, w_out, rows)

    heads = lax.axis_size("heads")
    first = part
    if is_power(heads) and heads > 1:
        mask = 1
        while True:
            received = swap(part, "heads", mask)
            mask *= 2
            if mask >= heads:
                break
            part = part + received
    else:
        part, received = lax.psum(part, "heads"), jnp.zeros_like(part)
    turned.append(fetch_turned(table, first, marks[2], marks[3], 3))
    turned.append(fetch_turned(table, part, marks[3], marks[4], 6))

    parts = [(part_, True, low) for part_, low in zip(turned, marks)]
    updated, scaled, piece, late_part = vocab_head(
        part, received, hidden_in, final_gain, parts, spans[0], table, (0, marks[0])
    )
    pairs = [pair_sum(piece, "seq")]
    piece = vocab_more(scaled, parts + [(late_part, False, 0)], spans[1])
    own, other = pair_sum(piece, "seq")
    *logits, front_stats, new_hidden = vocab_front(
        pairs, spans[:1], draft_ids, columns, features, updated
    )
    back, stats = vocab_back(own, other, front_stats, spans[1])
    if is_power(heads):
        every = [stats]
        for mask in range(1, heads):
            every.append(swap(stats, "heads", mask))
    else:
        gathered = lax.all_gather(stats, "heads")
        every = [gathered[i] for i in range(heads)]
        while not is_power(len(every)):
            every.append(jnp.concatenate([jnp.full_like(stats[:, :1], NEGATIVE), jnp.zeros_like(stats[:, 1:])], axis=1))
    log_probs, draft = vocab_finish(logits + [back], spans, every)
    return (new_hidden, log_probs, draft.reshape(rows))


def solution(mesh):
    return jax.shard_map(
        body,
        mesh=mesh,
        in_specs=(
            P("batch", "seq"),
            P("batch"),
            P("batch"),
            P("seq"),
            P("seq", "heads"),
            P("seq", "heads", None),
            P("batch", "heads", "seq", None),
            P("heads", None, None),
            P("heads", None, None),
            P("heads", "seq"),
            P("seq"),
            P("seq", "heads"),
        ),
        out_specs=(P("batch", "seq"), P("batch", "heads"), P("batch")),
        check_vma=False,
    )
```
